768 devices in a mesh: gx: 48 (over x, z), gy: 2 (over core), gz: 8 (over y).
Axes of the slice: x: 4, y: 8, z: 12, core: 2. Of those that a mesh axis runs over, the one named last changes fastest.
Arguments:
- density: int32 [192, 32, 1024], P('gx', 'gy', 'gz'), may hold values from 0 to 15
- fixed_mask: int32 [192, 32, 1024], P('gx', 'gy', 'gz'), may hold values from 0 to 1, as said below
- load_mask: int32 [192, 32, 1024], P('gx', 'gy', 'gz'), may hold values 0 or 1
- forces: float32 [3, 192, 32, 1024], P(None, 'gx', 'gy', 'gz'), may hold values from -6 to 6
Outputs:
- displacement: float32 [3, 192, 32, 1024], P(None, 'gx', 'gy', 'gz')
- residual: float32 [3, 192, 32, 1024], P(None, 'gx', 'gy', 'gz')
The draws below stay inside these ranges and needn't reach their ends.
Inputs may be any that keep to these rules, and one draw needn't show every extreme that they name: `fixed_mask`: supports stand only on voxels whose first index is 0 or 1.
All inputs are finite; a program needn't handle non-finite values. No bound on the sum of `load_mask` on one device may be relied on, other than what follows from the above.
Results may differ from the reference program's by a relative error of at most 0.0003.
Values sent between devices are 32-bit elements; how exact they have to be, the bound alone decides.
A program may use at most 32 MiB of HBM per device.

```python
import math
import jax
import jax.numpy as jnp
from jax import lax

CX = 4
ITERS = 2
NX = 192
NY = 32
NZ = 1024
N_GX = 48


def draw_fixed_mask(key, part):
    coin_key = jax.random.fold_in(key, 101)
    planes = jnp.arange(NX, dtype=jnp.int32)[:, None, None]
    coins = jax.random.randint(coin_key, (NX, NY, NZ), 0, 2, dtype=jnp.int32)
    return jnp.where(planes < 2, coins, 0).astype(jnp.int32)


def draw_forces(key, part):
    base_key = jax.random.fold_in(key, 211)
    rough_key, size_key, sign_key, phase_key = jax.random.split(base_key, 4)
    rough = jax.random.normal(rough_key, (3, NX, NY, NZ), jnp.float32)
    level = jax.random.uniform(size_key, (3,), jnp.float32, 0.02, 0.05)
    flips = jax.random.randint(sign_key, (3,), 0, 2, dtype=jnp.int32)
    signs = jnp.where(flips == 0, -1.0, 1.0).astype(jnp.float32)
    phases = jax.random.uniform(phase_key, (3,), jnp.float32, 0.0, 2.0 * math.pi)
    places = jnp.arange(NX, dtype=jnp.float32) / NX
    smooth = (signs * level)[:, None] * (1.0 + 0.5 * jnp.sin(2.0 * math.pi * places[None, :] + phases[:, None]))
    return jnp.clip(rough + smooth[:, :, None, None], -6.0, 6.0).astype(jnp.float32)


def set_ends(result, key, least, high):
    shape = result.shape
    index_at = [jax.random.randint(jax.random.fold_in(key, axis), (), 0, shape[axis]) for axis in range(len(shape))]
    result = result.at[tuple(index_at)].set(least)
    longest = shape.index(max(shape))
    index_at[longest] = (index_at[longest] + 1) % shape[longest]
    return result.at[tuple(index_at)].set(high)


def setup_inputs(seed: int = 0) -> dict:
    key_list = jax.random.split(jax.random.key(seed), 5)
    return {
        "density": set_ends(jax.random.randint(key_list[0], (NX, NY, NZ), 0, 16), jax.random.fold_in(key_list[0], 1), 0, 15).astype(jnp.int32),
        "fixed_mask": draw_fixed_mask(jax.random.fold_in(key_list[4], 71), 0),
        "load_mask": set_ends((jax.random.randint(key_list[2], (NX, NY, NZ), 0, 4) < 1).astype(jnp.int32), jax.random.fold_in(key_list[2], 1), 0, 1),
        "forces": draw_forces(jax.random.fold_in(key_list[4], 71), 0),
    }


LAME = 0.5
PENALTY = 4.0
OMEGA = 0.5
unit_steps = ((1, 0, 0), (0, 1, 0), (0, 0, 1))

def modulus(density):
    level = density.astype(jnp.float32) / 15.0
    return 0.05 + 0.95 * level * level * level

def shifted(padded, step_x, step_y, step_z):
    size_x = padded.shape[-3] - 2
    size_y = padded.shape[-2] - 2
    size_z = padded.shape[-1] - 2
    return padded[..., 1 + step_x:1 + step_x + size_x, 1 + step_y:1 + step_y + size_y, 1 + step_z:1 + step_z + size_z]

def stiffness_padded(padded, mod_pad, fixed_on):
    size_x = padded.shape[-3] - 2
    size_y = padded.shape[-2] - 2
    size_z = padded.shape[-1] - 2
    centre = shifted(padded, 0, 0, 0)
    centre_mod = shifted(mod_pad, 0, 0, 0)
    laplace = jnp.zeros_like(centre)
    for offsets in unit_steps:
        for parity in (1, -1):
            moved_x, moved_y, moved_z = (parity * offsets[0], parity * offsets[1], parity * offsets[2])
            coupling = 0.5 * (centre_mod + shifted(mod_pad, moved_x, moved_y, moved_z))
            laplace = laplace + coupling * (centre - shifted(padded, moved_x, moved_y, moved_z))
    spread = jnp.zeros(padded.shape[:-4] + (size_x + 1, size_y + 1, size_z + 1), jnp.float32)
    for component in range(3):
        offsets = unit_steps[component]
        plane = padded[..., component, :, :, :]
        spread = spread + plane[..., offsets[0]:offsets[0] + size_x + 1, offsets[1]:offsets[1] + size_y + 1, offsets[2]:offsets[2] + size_z + 1]
        spread = spread - plane[..., 0:size_x + 1, 0:size_y + 1, 0:size_z + 1]
    stress = mod_pad[0:size_x + 1, 0:size_y + 1, 0:size_z + 1] * spread
    upper_part = stress[..., 1:, 1:, 1:]
    pieces = []
    for component in range(3):
        offsets = unit_steps[component]
        lower_part = stress[..., 1 - offsets[0]:1 - offsets[0] + size_x, 1 - offsets[1]:1 - offsets[1] + size_y, 1 - offsets[2]:1 - offsets[2] + size_z]
        pieces.append(lower_part - upper_part)
    grad_div = jnp.stack(pieces, axis=-4)
    return laplace + LAME * grad_div + PENALTY * fixed_on * centre

def diagonal_of(mod_pad, fixed_on):
    centre_mod = shifted(mod_pad, 0, 0, 0)
    total = jnp.zeros_like(centre_mod)
    for offsets in unit_steps:
        for parity in (1, -1):
            total = total + 0.5 * (centre_mod + shifted(mod_pad, parity * offsets[0], parity * offsets[1], parity * offsets[2]))
    pieces = []
    for offsets in unit_steps:
        lower_mod = shifted(mod_pad, -offsets[0], -offsets[1], -offsets[2])
        pieces.append(total + LAME * (centre_mod + lower_mod) + PENALTY * fixed_on)
    return jnp.stack(pieces, axis=0)

def coarse_solve(factor, rhs_vec):
    lower_sol = lax.linalg.triangular_solve(factor, rhs_vec[:, None], left_side=True, lower=True)
    return lax.linalg.triangular_solve(factor, lower_sol, left_side=True, lower=True, transpose_a=True)[:, 0]

def reference(density, fixed_mask, load_mask, forces):
    modulus_field = modulus(density)
    mod_pad = jnp.pad(modulus_field, 1)
    fixed_on = fixed_mask.astype(jnp.float32)
    diagonal = diagonal_of(mod_pad, fixed_on)
    load_field = forces * (0.25 + load_mask.astype(jnp.float32))[None]

    def stiffness(trial_field):
        return stiffness_padded(jnp.pad(trial_field, ((0, 0), (1, 1), (1, 1), (1, 1))), mod_pad, fixed_on)
    slab_ids = jnp.arange(NX, dtype=jnp.int32) // CX

    def colour_sums(index):
        colour = (slab_ids % 3 == index // 3).astype(jnp.float32)
        choose = (jnp.arange(3, dtype=jnp.int32) == index % 3).astype(jnp.float32)
        trial_field = choose[:, None, None, None] * colour[None, :, None, None] * jnp.ones((1, 1, NY, NZ), jnp.float32)
        image_field = stiffness(trial_field)
        return image_field.reshape(3, N_GX, CX, NY, NZ).sum(axis=(2, 3, 4))
    colour_totals = lax.map(colour_sums, jnp.arange(9, dtype=jnp.int32)).reshape(3, 3, 3, N_GX)
    row_ids = jnp.arange(N_GX, dtype=jnp.int32)[:, None]
    col_ids = jnp.arange(N_GX, dtype=jnp.int32)[None, :]
    adjacent = jnp.abs(col_ids - row_ids) <= 1
    coarse = jnp.zeros((N_GX, 3, N_GX, 3), jnp.float32)
    for colour_id in range(3):
        colour_mask = (adjacent & (col_ids % 3 == colour_id)).astype(jnp.float32)
        block_vals = jnp.transpose(colour_totals[colour_id], (2, 1, 0))
        coarse = coarse + colour_mask[:, None, :, None] * block_vals[:, :, None, :]
    factor = jnp.linalg.cholesky(coarse.reshape(3 * N_GX, 3 * N_GX))

    def precondition(residual):
        smooth_one = OMEGA * residual / diagonal
        after_one = residual - stiffness(smooth_one)
        slab_totals = after_one.reshape(3, N_GX, CX, NY, NZ).sum(axis=(2, 3, 4)).T
        correction = coarse_solve(factor, slab_totals.reshape(-1)).reshape(N_GX, 3)
        smooth_two = smooth_one + jnp.repeat(correction.T, CX, axis=1)[:, :, None, None]
        return smooth_two + OMEGA * (residual - stiffness(smooth_two)) / diagonal
    solution = jnp.zeros_like(load_field)
    residual = load_field
    precond = precondition(residual)
    search = precond
    norm_now = jnp.sum(residual * precond)
    for iteration in range(ITERS):
        image_field = stiffness(search)
        step_size = norm_now / jnp.sum(search * image_field)
        solution = solution + step_size * search
        residual = residual - step_size * image_field
        if iteration + 1 < ITERS:
            precond = precondition(residual)
            norm_next = jnp.sum(residual * precond)
            search = precond + norm_next / norm_now * search
            norm_now = norm_next
    return (solution, residual)
```

```python
import jax
import jax.numpy as jnp
from jax import lax
from jax.experimental import pallas as pl
from jax.experimental.pallas import tpu as pltpu
from jax.sharding import PartitionSpec as P

LAME = 0.5
PENALTY = 4.0
OMEGA = 0.5
F32 = jnp.float32
MESH = pl.DeviceIdType.MESH
LANES = 128
N_MSG = 9
N_EX = 5


def steps_for(count):
    steps = 0
    while (1 << steps) < count:
        steps += 1
    return steps


def kernel(
    sizes,
    density,
    fixed_mask,
    load_mask,
    forces,
    disp_out,
    res_out,
    mod_buf,
    fields,
    low_z,
    high_z,
    mod_low,
    pack_send,
    pack_recv,
    edge_recv,
    stress,
    coef,
    dinv_buf,
    keep,
    rows_buf,
    pcr_buf,
    row_send,
    group_recv,
    slab_recv,
    halo_send_sem,
    halo_recv_sem,
    row_send_sem,
    row_recv_sem,
):
    n_gx, n_gy, n_gz = sizes
    n_group = n_gy * n_gz
    gx, gy, gz = (lax.axis_index("gx"), lax.axis_index("gy"), lax.axis_index("gz"))

    def wrap(value, count):
        value = jnp.where(value >= count, value - count, value)
        return jnp.where(value < 0, value + count, value)

    gx_up, gx_dn = (wrap(gx + 1, n_gx), wrap(gx - 1, n_gx))
    gz_up, gz_dn = (wrap(gz + 1, n_gz), wrap(gz - 1, n_gz))
    gy_other = 1 - gy
    gx_side = wrap(gx + 2 * gy - 1, n_gx)
    gz_side = wrap(gz + 2 * gy - 1, n_gz)

    def group_member(step):
        y_at = jnp.where(step >= n_gz, gy_other, gy)
        z_at = wrap(gz + jnp.where(step >= n_gz, step - n_gz, step), n_gz)
        return (gx, y_at, z_at)

    barrier = pltpu.get_barrier_semaphore()

    def greet(where_to):
        pl.semaphore_signal(barrier, inc=1, device_id=where_to, device_id_type=MESH)

    def greet_slab(step, carry):
        greet((wrap(gx + step, n_gx), gy, gz))
        return carry

    def greet_group(step, carry):
        greet(group_member(step))
        return carry

    greet((gx_side, gy_other, gz))
    greet((gx_dn, gy, gz_up))
    greet((gx_up, gy, gz_dn))
    lax.fori_loop(1, n_gx, greet_slab, 0)
    lax.fori_loop(1, n_group, greet_group, 0)

    has_xm = jnp.where(gx > 0, 1.0, 0.0).astype(F32)
    has_xp = jnp.where(gx < n_gx - 1, 1.0, 0.0).astype(F32)
    has_zm = jnp.where(gz > 0, 1.0, 0.0).astype(F32)
    has_zp = jnp.where(gz < n_gz - 1, 1.0, 0.0).astype(F32)
    is_y0 = jnp.where(gy == 0, 1.0, 0.0).astype(F32)
    is_y1 = 1.0 - is_y0

    shape = (4, 16, LANES)
    lane3 = lax.broadcasted_iota(jnp.int32, shape, 2)
    x3 = lax.broadcasted_iota(jnp.int32, shape, 0)
    y3 = lax.broadcasted_iota(jnp.int32, shape, 1)
    slot3 = 2 * x3 + jnp.where(y3 >= 8, 1, 0)
    first_lane, last_lane = (lane3 == 0, lane3 == LANES - 1)
    wide_lane = lax.broadcasted_iota(jnp.int32, (5, 24, LANES), 2) == LANES - 1
    lane2 = lax.broadcasted_iota(jnp.int32, (16, LANES), 1)
    diag2 = lane2 == lax.broadcasted_iota(jnp.int32, (16, LANES), 0)

    zeros_side = jnp.zeros((4, 8, LANES), F32)
    outside = pl.ds(pl.multiple_of(24 * gy, 8), 8)
    for buf, count in [(mod_buf, 1)] + [(fields.at[e], 3) for e in range(N_EX - 1)]:
        for c in range(count):
            buf[c, 1:5, outside, :] = zeros_side

    level = density[...].astype(F32) / 15.0
    mod = 0.05 + 0.95 * level * level * level
    mod_buf[0, 1:5, 8:24, :] = mod
    fixed4 = PENALTY * fixed_mask[...].astype(F32)
    load_scale = 0.25 + load_mask[...].astype(F32)
    load = [forces[c] * load_scale for c in range(3)]

    def pack_side(values, lane):
        total = None
        for c, value in enumerate(values):
            spread = jnp.broadcast_to(value[:, :, lane : lane + 1], shape)
            chosen = jnp.where(lane3 == slot3 + 8 * c, spread, 0.0)
            flat = chosen[0] + chosen[1] + chosen[2] + chosen[3]
            part = flat[0:8] + flat[8:16]
            total = part if total is None else total + part
        return total

    def remote(e, k, src, dst, where_to):
        copy = pltpu.make_async_remote_copy(
            src_ref=src,
            dst_ref=dst,
            send_sem=halo_send_sem.at[e, k],
            recv_sem=halo_recv_sem.at[e, k],
            device_id=where_to,
            device_id_type=MESH,
        )
        copy.start()
        return copy

    def start_halo(e, buf, values, with_edges):
        copies = [
            remote(e, 0, buf.at[:, 4, 8:24, :], buf.at[:, 0, 8:24, :], (gx_up, gy, gz)),
            remote(e, 1, buf.at[:, 1, 8:24, :], buf.at[:, 5, 8:24, :], (gx_dn, gy, gz)),
        ]
        pack_send[e, 0] = pack_side(values, LANES - 1)
        pack_send[e, 1] = pack_side(values, 0)
        copies.append(
            remote(e, 2, pack_send.at[e, 0], pack_recv.at[e, 0], (gx, gy, gz_up))
        )
        copies.append(
            remote(e, 3, pack_send.at[e, 1], pack_recv.at[e, 1], (gx, gy, gz_dn))
        )
        if with_edges:
            copies.append(
                remote(e, 4, pack_send.at[e, 0], pack_recv.at[e, 2], (gx_dn, gy, gz_up))
            )
            copies.append(
                remote(e, 5, pack_send.at[e, 1], pack_recv.at[e, 3], (gx_up, gy, gz_dn))
            )
            copies.append(
                remote(
                    e, 6, pack_send.at[e, 1 - gy], pack_recv.at[e, 4], (gx, gy_other, gz_side)
                )
            )
            copies.append(
                remote(
                    e,
                    7,
                    buf.at[gy, 1 + 3 * gy, pl.ds(pl.multiple_of(16 - 8 * gy, 8), 8), :],
                    edge_recv.at[e],
                    (gx_side, gy_other, gz),
                )
            )
        copies.append(
            remote(
                e,
                8,
                buf.at[:, 1:5, pl.ds(pl.multiple_of(16 - 8 * gy, 8), 8), :],
                buf.at[:, 1:5, pl.ds(pl.multiple_of(24 * gy, 8), 8), :],
                (gx, gy_other, gz),
            )
        )
        return copies

    def finish_halo(e, buf, copies, with_edges):
        for copy in copies:
            copy.wait()
        count = buf.shape[0]
        for c in range(count):
            buf[c, 0, 8:24, :] = buf[c, 0, 8:24, :] * has_xm
            buf[c, 5, 8:24, :] = buf[c, 5, 8:24, :] * has_xp
        low = pack_recv[e, 0] * has_zm
        high = pack_recv[e, 1] * has_zp
        target_low = low_z if with_edges else mod_low
        target_high = high_z
        for c in range(count):
            for x in range(4):
                for t in range(2):
                    j = 8 * c + 2 * x + t
                    rows = slice(8 + 8 * t, 16 + 8 * t)
                    target_low[c, 1 + x, rows, :] = jnp.broadcast_to(low[:, j : j + 1], (8, LANES))
                    target_high[c, 1 + x, rows, :] = jnp.broadcast_to(
                        high[:, j : j + 1], (8, LANES)
                    )
        if with_edges:
            low_x = pack_recv[e, 2] * (has_xp * has_zm)
            high_x = pack_recv[e, 3] * (has_xm * has_zp)
            side = pack_recv[e, 4]
            low_y = side * (is_y0 * has_zm)
            high_y = side * (is_y1 * has_zp)
            for t in range(2):
                rows = slice(8 + 8 * t, 16 + 8 * t)
                j = t
                low_z[0, 5, rows, :] = jnp.broadcast_to(low_x[:, j : j + 1], (8, LANES))
                j = 8 * 2 + 2 * 3 + t
                high_z[2, 0, rows, :] = jnp.broadcast_to(high_x[:, j : j + 1], (8, LANES))
            for x in range(4):
                j = 8 + 2 * x
                low_z[1, 1 + x, 24:32, :] = jnp.broadcast_to(low_y[:, j : j + 1], (8, LANES))
                j = 8 * 2 + 2 * x + 1
                high_z[2, 1 + x, 0:8, :] = jnp.broadcast_to(high_y[:, j : j + 1], (8, LANES))
            corner = edge_recv[e]
            buf[1, 0, 24:32, :] = corner * (is_y0 * has_xm)
            buf[0, 5, 0:8, :] = corner * (is_y1 * has_xp)

    def before(value, low):
        return jnp.where(first_lane, low, pltpu.roll(value, 1, 2))

    def after(value, high):
        return jnp.where(last_lane, high, pltpu.roll(value, LANES - 1, 2))

    def set_field(e, values):
        for c in range(3):
            fields[e, c, 1:5, 8:24, :] = values[c]

    def stiffness(e):
        buf = fields.at[e]
        u_z = buf[2, 0:5, 0:24, :]
        up_z = jnp.where(wide_lane, high_z[2, 0:5, 0:24, :], pltpu.roll(u_z, LANES - 1, 2))
        spread = (
            (buf[0, 1:6, 0:24, :] - buf[0, 0:5, 0:24, :])
            + (buf[1, 0:5, 1:25, :] - buf[1, 0:5, 0:24, :])
            + (up_z - u_z)
        )
        stress[...] = mod_buf[0, 0:5, 0:24, :] * spread
        here = stress[1:5, 8:24, :]
        spread_low = (
            (low_z[0, 2:6, 8:24, :] - low_z[0, 1:5, 8:24, :])
            + (low_z[1, 1:5, 9:25, :] - low_z[1, 1:5, 8:24, :])
            + (buf[2, 1:5, 8:24, :] - low_z[2, 1:5, 8:24, :])
        )
        below = [
            stress[0:4, 8:24, :],
            stress[1:5, 7:23, :],
            before(here, mod_low[0, 1:5, 8:24, :] * spread_low),
        ]
        images = []
        for c in range(3):
            centre = buf[c, 1:5, 8:24, :]
            image = coef[6] * centre
            image = image - coef[0] * buf[c, 0:4, 8:24, :]
            image = image - coef[1] * buf[c, 2:6, 8:24, :]
            image = image - coef[2] * buf[c, 1:5, 7:23, :]
            image = image - coef[3] * buf[c, 1:5, 9:25, :]
            image = image - coef[4] * before(centre, low_z[c, 1:5, 8:24, :])
            image = image - coef[5] * after(centre, high_z[c, 1:5, 8:24, :])
            images.append(image + LAME * (below[c] - here))
        return images

    def put_sum(q, value):
        if value.ndim == 3:
            value = value[0] + value[1] + value[2] + value[3]
        value = value[0:8] + value[8:16]
        rows_buf[q : q + 1, :] = jnp.sum(value, axis=0, keepdims=True)

    def make_row():
        sums = jnp.sum(rows_buf[...], axis=1, keepdims=True)
        return jnp.sum(jnp.where(diag2, sums, 0.0), axis=0, keepdims=True)

    me_group = gy * n_gz + gz

    def gather_rows(i, row):
        row_send[i, 0] = row
        group_recv[i, me_group] = row

        def group_copy(step):
            return pltpu.make_async_remote_copy(
                src_ref=row_send.at[i, 0],
                dst_ref=group_recv.at[i, me_group],
                send_sem=row_send_sem.at[i, 0],
                recv_sem=row_recv_sem.at[i, 0],
                device_id=group_member(step),
                device_id_type=MESH,
            )

        def start_group(step, carry):
            group_copy(step).start()
            return carry

        lax.fori_loop(1, n_group, start_group, 0)
        most = group_recv.at[i, pl.ds(0, n_group - 1)]
        pltpu.make_async_copy(most, most, row_recv_sem.at[i, 0]).wait()
        total = group_recv[i, 0]
        for k in range(1, n_group):
            total = total + group_recv[i, k]
        row_send[i, 1] = total
        slab_recv[i, gx] = total

        def start_slab(step, carry):
            pltpu.make_async_remote_copy(
                src_ref=row_send.at[i, 1],
                dst_ref=slab_recv.at[i, gx],
                send_sem=row_send_sem.at[i, 1],
                recv_sem=row_recv_sem.at[i, 1],
                device_id=(wrap(gx + step, n_gx), gy, gz),
                device_id_type=MESH,
            ).start()
            return carry

        lax.fori_loop(1, n_gx, start_slab, 0)
        rest = slab_recv.at[i, pl.ds(0, n_gx - 1)]
        pltpu.make_async_copy(rest, rest, row_recv_sem.at[i, 1]).wait()
        pltpu.make_async_copy(most, most, row_send_sem.at[i, 0]).wait()
        pltpu.make_async_copy(rest, rest, row_send_sem.at[i, 1]).wait()

    def slab_rows(i):
        table = jnp.concatenate(
            [slab_recv[i, k] for k in range(n_gx)]
            + [jnp.zeros((LANES - n_gx, LANES), F32)],
            axis=0,
        )
        return jnp.transpose(table)

    lane_row = lax.broadcasted_iota(jnp.int32, (1, LANES), 1)
    sub8 = lax.broadcasted_iota(jnp.int32, (8, LANES), 0)
    n_steps = steps_for(n_gx)

    def stack3(a, b, c):
        return jnp.where(sub8 == 0, a, jnp.where(sub8 == 1, b, jnp.where(sub8 == 2, c, 0.0)))

    def times(matrix, column):
        return (
            matrix[0] * column[0:1, :] + matrix[1] * column[1:2, :] + matrix[2] * column[2:3, :]
        )

    def inverse(cols):
        a, d, g = (cols[0][0:1, :], cols[0][1:2, :], cols[0][2:3, :])
        b, e, h = (cols[1][0:1, :], cols[1][1:2, :], cols[1][2:3, :])
        c, f, i = (cols[2][0:1, :], cols[2][1:2, :], cols[2][2:3, :])
        m00, m01, m02 = (e * i - f * h, c * h - b * i, b * f - c * e)
        m10, m11, m12 = (f * g - d * i, a * i - c * g, c * d - a * f)
        m20, m21, m22 = (d * h - e * g, b * g - a * h, a * e - b * d)
        scale = 1.0 / (a * m00 + b * m10 + c * m20)
        return [
            stack3(m00 * scale, m10 * scale, m20 * scale),
            stack3(m01 * scale, m11 * scale, m21 * scale),
            stack3(m02 * scale, m12 * scale, m22 * scale),
        ]

    def factorise(lower, main, upper, rhs):
        def body(step, carry):
            stride, low, mid, high, vec = carry
            back = LANES - stride
            inv = inverse(mid)
            inv_dn = [pltpu.roll(v, stride, 1) for v in inv]
            inv_up = [pltpu.roll(v, back, 1) for v in inv]
            alpha = [-times(low, v) for v in inv_dn]
            gamma = [-times(high, v) for v in inv_up]
            for k in range(3):
                pcr_buf[step, k] = alpha[k]
                pcr_buf[step, 3 + k] = gamma[k]
            low_dn = [pltpu.roll(v, stride, 1) for v in low]
            high_dn = [pltpu.roll(v, stride, 1) for v in high]
            low_up = [pltpu.roll(v, back, 1) for v in low]
            high_up = [pltpu.roll(v, back, 1) for v in high]
            vec_dn = pltpu.roll(vec, stride, 1)
            vec_up = pltpu.roll(vec, back, 1)
            new_mid = [
                mid[k] + times(alpha, high_dn[k]) + times(gamma, low_up[k]) for k in range(3)
            ]
            new_low = [times(alpha, v) for v in low_dn]
            new_high = [times(gamma, v) for v in high_up]
            new_vec = vec + times(alpha, vec_dn) + times(gamma, vec_up)
            return (stride * 2, new_low, new_mid, new_high, new_vec)

        _, _, mid, _, vec = lax.fori_loop(
            0, n_steps, body, (jnp.int32(1), lower, main, upper, rhs)
        )
        inv = inverse(mid)
        for k in range(3):
            pcr_buf[n_steps, k] = inv[k]
        return times(inv, vec)

    def solve_again(vec):
        stride = 1
        for step in range(n_steps):
            alpha = [pcr_buf[step, k] for k in range(3)]
            gamma = [pcr_buf[step, 3 + k] for k in range(3)]
            vec_dn = pltpu.roll(vec, stride, 1)
            vec_up = pltpu.roll(vec, LANES - stride, 1)
            vec = vec + times(alpha, vec_dn) + times(gamma, vec_up)
            stride *= 2
        return times([pcr_buf[n_steps, k] for k in range(3)], vec)

    def nearby(solved):
        turned = pltpu.roll(solved, wrap(1 - gx, LANES), 1)
        return [
            [jnp.broadcast_to(turned[c : c + 1, b : b + 1], (16, LANES)) for c in range(3)]
            for b in range(3)
        ]

    pl.semaphore_wait(barrier, n_gx - 1 + n_group - 1 + 3)

    copies = start_halo(0, mod_buf, [mod], False)
    finish_halo(0, mod_buf, copies, False)
    mod_zm = before(mod, mod_low[0, 1:5, 8:24, :])
    mod_zp = after(mod, high_z[0, 1:5, 8:24, :])
    mod_xm, mod_xp = (mod_buf[0, 0:4, 8:24, :], mod_buf[0, 2:6, 8:24, :])
    mod_ym, mod_yp = (mod_buf[0, 1:5, 7:23, :], mod_buf[0, 1:5, 9:25, :])
    couplings = [0.5 * (mod + v) for v in (mod_xm, mod_xp, mod_ym, mod_yp, mod_zm, mod_zp)]
    total = fixed4
    for k in range(6):
        coef[k] = couplings[k]
        total = total + couplings[k]
    coef[6] = total
    for c in range(3):
        dinv_buf[c] = OMEGA / (total + couplings[2 * c])

    first = [load[c] * dinv_buf[c] for c in range(3)]
    set_field(0, first)
    copies = start_halo(1, fields.at[0], first, True)

    low_y_edge = jnp.where(y3 == 0, is_y0, 0.0)
    high_y_edge = jnp.where(y3 == 15, is_y1, 0.0)
    low_z_edge = jnp.where(first_lane, 1.0 - has_zm, 0.0)
    high_z_edge = jnp.where(last_lane, 1.0 - has_zp, 0.0)
    first_x = jnp.where(x3 == 0, 1.0, 0.0)
    last_x = jnp.where(x3 == 3, 1.0, 0.0)
    bound = (
        fixed4
        + couplings[2] * low_y_edge
        + couplings[3] * high_y_edge
        + couplings[4] * low_z_edge
        + couplings[5] * high_z_edge
        + couplings[0] * first_x
        + couplings[1] * last_x
    )
    half = LAME * mod
    half_xm = LAME * mod_xm
    keep[0] = bound
    rows_buf[...] = jnp.zeros((16, LANES), F32)
    put_sum(0, bound + half_xm * first_x + half * last_x)
    put_sum(1, bound + half * high_y_edge)
    put_sum(2, bound + half * high_z_edge)
    put_sum(3, half[3] * high_y_edge[3])
    put_sum(4, half[3] * high_z_edge[3])
    put_sum(5, half * high_y_edge * high_z_edge)
    put_sum(6, couplings[1][3])
    put_sum(7, couplings[1][3] + half[3])

    def image_of(coarse):
        under, own, over = coarse
        bound = keep[0]
        mod = mod_buf[0, 1:5, 8:24, :]
        half = LAME * mod
        half_xm = LAME * mod_buf[0, 0:4, 8:24, :]
        half_ym = LAME * mod_buf[0, 1:5, 7:23, :]
        half_zm = LAME * before(mod, mod_low[0, 1:5, 8:24, :])
        low_x, high_x = (coef[0], coef[1])
        inner_xm = half_xm * (1.0 - first_x)
        down_y, down_z = (half - half_ym, half - half_zm)
        image_x = (
            (bound + half_xm * first_x + half * last_x) * own[0]
            + (half - inner_xm) * (high_y_edge * own[1] + high_z_edge * own[2])
            - first_x
            * (
                (low_x + half_xm) * under[0]
                + half_xm * (high_y_edge * under[1] + high_z_edge * under[2])
            )
            - last_x * (high_x + half) * over[0]
        )
        image_y = (
            (bound + half * high_y_edge) * own[1]
            + down_y * (last_x * (own[0] - over[0]) + high_z_edge * own[2])
            - first_x * low_x * under[1]
            - last_x * high_x * over[1]
        )
        image_z = (
            (bound + half * high_z_edge) * own[2]
            + down_z * (last_x * (own[0] - over[0]) + high_y_edge * own[1])
            - first_x * low_x * under[2]
            - last_x * high_x * over[2]
        )
        return [image_x, image_y, image_z]

    finish_halo(1, fields.at[0], copies, True)
    image_first = stiffness(0)
    rest = [load[c] - image_first[c] for c in range(3)]
    for c in range(3):
        put_sum(8 + c, rest[c])
        keep[1 + c] = rest[c]
    gather_rows(0, make_row())

    table = slab_rows(0)
    real = lane_row < n_gx
    row = [jnp.where(real, table[q : q + 1, :], 0.0) for q in range(11)]
    one = jnp.where(real, 0.0, 1.0)
    none = jnp.zeros((1, LANES), F32)
    main = [
        stack3(row[0] + one, row[3], row[4]),
        stack3(row[3], row[1] + one, row[5]),
        stack3(row[4], row[5], row[2] + one),
    ]
    joined = lane_row < n_gx - 1
    side = [jnp.where(joined, row[q], 0.0) for q in (7, 3, 4, 6)]
    upper = [
        stack3(-side[0], -side[1], -side[2]),
        stack3(none, -side[3], none),
        stack3(none, none, -side[3]),
    ]
    moved = [pltpu.roll(jnp.broadcast_to(v, (8, LANES)), 1, 1)[0:1, :] for v in side]
    lower = [
        stack3(-moved[0], none, none),
        stack3(-moved[1], -moved[3], none),
        stack3(-moved[2], none, -moved[3]),
    ]
    near = nearby(factorise(lower, main, upper, stack3(row[8], row[9], row[10])))
    coarse_image = image_of(near)
    precond = []
    for c in range(3):
        second = fields[0, c, 1:5, 8:24, :] + near[1][c]
        precond.append(second + dinv_buf[c] * (keep[1 + c] - coarse_image[c]))
    set_field(1, precond)
    copies = start_halo(2, fields.at[1], precond, True)
    load = [forces[c] * load_scale for c in range(3)]
    rows_buf[...] = jnp.zeros((16, LANES), F32)
    put_sum(0, load[0] * precond[0] + load[1] * precond[1] + load[2] * precond[2])
    finish_halo(2, fields.at[1], copies, True)
    image = stiffness(1)
    smooth = []
    for c in range(3):
        keep[4 + c] = image[c]
        smooth.append(dinv_buf[c] * image[c])
    set_field(2, smooth)
    copies = start_halo(3, fields.at[2], smooth, True)
    precond = [fields[1, c, 1:5, 8:24, :] for c in range(3)]
    put_sum(1, image[0] * precond[0] + image[1] * precond[1] + image[2] * precond[2])
    finish_halo(3, fields.at[2], copies, True)
    image_smooth = stiffness(2)
    for c in range(3):
        remain = keep[4 + c] - image_smooth[c]
        keep[1 + c] = remain
        put_sum(2 + c, remain)
    gather_rows(1, make_row())

    table = slab_rows(1)
    row = [jnp.where(real, table[q : q + 1, :], 0.0) for q in range(5)]
    norm_now = jnp.sum(row[0], axis=1, keepdims=True)
    curve = jnp.sum(row[1], axis=1, keepdims=True)
    step0 = norm_now / curve
    near = nearby(solve_again(stack3(row[2], row[3], row[4])))
    coarse_image = image_of(near)
    wide0 = jnp.broadcast_to(step0, (16, LANES))
    following = []
    for c in range(3):
        second = fields[2, c, 1:5, 8:24, :] + near[1][c]
        change = second + dinv_buf[c] * (keep[1 + c] - coarse_image[c])
        following.append(fields[1, c, 1:5, 8:24, :] - wide0 * change)
    set_field(3, following)
    copies = start_halo(4, fields.at[3], following, True)
    rows_buf[...] = jnp.zeros((16, LANES), F32)
    residual = []
    product = jnp.zeros(shape, F32)
    for c in range(3):
        residual.append(forces[c] * load_scale - wide0 * keep[4 + c])
        product = product + residual[c] * following[c]
        keep[1 + c] = residual[c]
    put_sum(0, product)
    finish_halo(4, fields.at[3], copies, True)
    image_next = stiffness(3)
    product = jnp.zeros(shape, F32)
    for c in range(3):
        product = product + image_next[c] * fields[3, c, 1:5, 8:24, :]
        keep[7 + c] = image_next[c]
    put_sum(1, product)
    gather_rows(2, make_row())

    both = slab_recv[2, 0]
    for k in range(1, n_gx):
        both = both + slab_recv[2, k]
    norm_next, curve_next = (both[0:1, 0:1], both[0:1, 1:2])
    ratio = norm_next / norm_now
    step1 = norm_next / (curve_next - ratio * norm_next / step0)
    wide_ratio = jnp.broadcast_to(ratio, (16, LANES))
    wide1 = jnp.broadcast_to(step1, (16, LANES))
    for c in range(3):
        previous = fields[1, c, 1:5, 8:24, :]
        search = fields[3, c, 1:5, 8:24, :] + wide_ratio * previous
        disp_out[c] = wide0 * previous + wide1 * search
        res_out[c] = keep[1 + c] - wide1 * (keep[7 + c] + wide_ratio * keep[4 + c])


def solution(mesh):
    sizes = tuple(mesh.shape[name] for name in ("gx", "gy", "gz"))
    n_gx, n_gy, n_gz = sizes
    n_group = n_gy * n_gz
    block = jax.ShapeDtypeStruct((3, 4, 16, LANES), F32)
    vmem = pl.BlockSpec(memory_space=pltpu.VMEM)

    def body(density, fixed_mask, load_mask, forces):
        def run(*refs):
            kernel(sizes, *refs)

        return pl.pallas_call(
            run,
            out_shape=(block, block),
            in_specs=[vmem] * 4,
            out_specs=(vmem, vmem),
            scratch_shapes=[
                pltpu.VMEM((1, 6, 32, LANES), F32),
                pltpu.VMEM((N_EX - 1, 3, 6, 32, LANES), F32),
                pltpu.VMEM((3, 6, 32, LANES), F32),
                pltpu.VMEM((3, 6, 32, LANES), F32),
                pltpu.VMEM((1, 6, 32, LANES), F32),
                pltpu.VMEM((N_EX, 2, 8, LANES), F32),
                pltpu.VMEM((N_EX, 5, 8, LANES), F32),
                pltpu.VMEM((N_EX, 8, LANES), F32),
                pltpu.VMEM((5, 24, LANES), F32),
                pltpu.VMEM((7, 4, 16, LANES), F32),
                pltpu.VMEM((3, 4, 16, LANES), F32),
                pltpu.VMEM((10, 4, 16, LANES), F32),
                pltpu.VMEM((16, LANES), F32),
                pltpu.VMEM((steps_for(n_gx) + 1, 6, 8, LANES), F32),
                pltpu.VMEM((3, 2, 1, LANES), F32),
                pltpu.VMEM((3, n_group, 1, LANES), F32),
                pltpu.VMEM((3, n_gx, 1, LANES), F32),
                pltpu.SemaphoreType.DMA((N_EX, N_MSG)),
                pltpu.SemaphoreType.DMA((N_EX, N_MSG)),
                pltpu.SemaphoreType.DMA((3, 2)),
                pltpu.SemaphoreType.DMA((3, 2)),
            ],
            compiler_params=pltpu.CompilerParams(collective_id=0, has_side_effects=True),
        )(density, fixed_mask, load_mask, forces)

    spec = P("gx", "gy", "gz")
    wide = P(None, "gx", "gy", "gz")
    return jax.shard_map(
        body,
        mesh=mesh,
        in_specs=(spec, spec, spec, wide),
        out_specs=(wide, wide),
        check_vma=False,
    )
```

```python
import jax
import jax.numpy as jnp
from jax import lax
from jax.experimental import pallas as pl
from jax.experimental.pallas import tpu as pltpu
from jax.sharding import PartitionSpec as P

LAME = 0.5
PENALTY = 4.0
OMEGA = 0.5
F32 = jnp.float32
MESH = pl.DeviceIdType.MESH
LANES = 128
N_MSG = 9
N_EX = 6
N_FIELD = 4
N_BASIS = 10


def steps_for(count):
    steps = 0
    while (1 << steps) < count:
        steps += 1
    return steps


def kernel(
    sizes,
    density,
    fixed_mask,
    load_mask,
    forces,
    disp_out,
    res_out,
    mod_buf,
    fields,
    low_all,
    high_all,
    mod_low,
    mod_high,
    basis,
    basis_low,
    basis_high,
    pack_send,
    pack_recv,
    edge_recv,
    basis_edge,
    stress,
    coef,
    dinv_buf,
    keep,
    rows_buf,
    pcr_buf,
    row_send,
    group_recv,
    slab_recv,
    in_density,
    in_fixed,
    in_load,
    in_forces,
    in_sem,
    halo_send_sem,
    halo_recv_sem,
    row_send_sem,
    row_recv_sem,
    flood_sem,
):
    n_gx, n_gy, n_gz = sizes
    n_group = n_gy * n_gz
    gx, gy, gz = (lax.axis_index("gx"), lax.axis_index("gy"), lax.axis_index("gz"))

    def wrap(value, count):
        value = jnp.where(value >= count, value - count, value)
        return jnp.where(value < 0, value + count, value)

    gx_up, gx_dn = (wrap(gx + 1, n_gx), wrap(gx - 1, n_gx))
    gz_up, gz_dn = (wrap(gz + 1, n_gz), wrap(gz - 1, n_gz))
    gy_other = 1 - gy
    gx_side = wrap(gx + 2 * gy - 1, n_gx)
    gz_side = wrap(gz + 2 * gy - 1, n_gz)

    def group_member(step):
        y_at = jnp.where(step >= n_gz, gy_other, gy)
        z_at = wrap(gz + jnp.where(step >= n_gz, step - n_gz, step), n_gz)
        return (gx, y_at, z_at)

    barrier = pltpu.get_barrier_semaphore()

    def greet(where_to):
        pl.semaphore_signal(barrier, inc=1, device_id=where_to, device_id_type=MESH)

    near = [
        (gx_up, gy, gz),
        (gx_dn, gy, gz),
        (gx, gy, gz_up),
        (gx, gy, gz_dn),
        (gx, gy_other, gz),
        (gx_side, gy_other, gz),
        (gx_dn, gy, gz_up),
        (gx_up, gy, gz_dn),
        (gx, gy_other, gz_side),
    ]
    n_fast = 12 if n_gx == 48 else n_gx
    n_slow = n_gx // n_fast
    slow = gx // n_fast
    fast = gx - slow * n_fast
    ring_fast = [slow * n_fast + wrap(fast + d, n_fast) for d in (1, -1)]
    ring_slow = [wrap(slow + d, n_slow) * n_fast + fast for d in (1, -1)]
    if n_slow > 1:
        near = near + [(v, gy, gz) for v in ring_slow + ring_fast]
    for where_to in near:
        greet(where_to)
    fetches = []
    for k, (src, dst) in enumerate(
        ((density, in_density), (fixed_mask, in_fixed), (load_mask, in_load), (forces, in_forces))
    ):
        fetch = pltpu.make_async_copy(src, dst, in_sem.at[k])
        fetch.start()
        fetches.append(fetch)

    ring_y = [(gx, gy, gz_up), (gx, gy, gz_dn)]
    ring_z = [(v, gy, gz) for v in ring_fast]
    ring_x = [(v, gy, gz) for v in ring_slow]
    n_y, n_z = (max(n_gz // 2 - 1, 0), max(n_fast // 2 - 1, 0))
    floods = []
    for k in range(max(n_y, n_z)):
        floods.append(([ring_y] if k < n_y else []) + ([ring_z] if k < n_z else []))
    if n_slow > 1:
        floods += [[ring_x]] * max(n_slow // 2, 1)

    def flood(first, last):
        for k in range(first, min(last, len(floods))):
            for r, ring in enumerate(floods[k]):
                for where_to in ring:
                    pl.semaphore_signal(
                        flood_sem.at[k, r], inc=1, device_id=where_to, device_id_type=MESH
                    )
            for r in range(len(floods[k])):
                pl.semaphore_wait(flood_sem.at[k, r], 2)

    has_xm = jnp.where(gx > 0, 1.0, 0.0).astype(F32)
    has_xp = jnp.where(gx < n_gx - 1, 1.0, 0.0).astype(F32)
    has_zm = jnp.where(gz > 0, 1.0, 0.0).astype(F32)
    has_zp = jnp.where(gz < n_gz - 1, 1.0, 0.0).astype(F32)
    is_y0 = jnp.where(gy == 0, 1.0, 0.0).astype(F32)
    is_y1 = 1.0 - is_y0

    shape = (4, 16, LANES)
    lane3 = lax.broadcasted_iota(jnp.int32, shape, 2)
    x3 = lax.broadcasted_iota(jnp.int32, shape, 0)
    y3 = lax.broadcasted_iota(jnp.int32, shape, 1)
    slot3 = 2 * x3 + jnp.where(y3 >= 8, 1, 0)
    first_lane, last_lane = (lane3 == 0, lane3 == LANES - 1)
    wide_lane = lax.broadcasted_iota(jnp.int32, (5, 24, LANES), 2) == LANES - 1
    lane2 = lax.broadcasted_iota(jnp.int32, (16, LANES), 1)
    diag2 = lane2 == lax.broadcasted_iota(jnp.int32, (16, LANES), 0)

    zeros_side = jnp.zeros((4, 8, LANES), F32)
    outside = pl.ds(pl.multiple_of(24 * gy, 8), 8)
    padded = [(mod_buf, 1), (basis, N_BASIS)] + [(fields.at[e], 3) for e in range(N_FIELD)]
    for buf, count in padded:
        for c in range(count):
            buf[c, 1:5, outside, :] = zeros_side

    for fetch in fetches:
        fetch.wait()
    level = in_density[...].astype(F32) / 15.0
    mod = 0.05 + 0.95 * level * level * level
    mod_buf[0, 1:5, 8:24, :] = mod
    fixed4 = PENALTY * in_fixed[...].astype(F32)
    load_scale = 0.25 + in_load[...].astype(F32)
    load = [in_forces[c] * load_scale for c in range(3)]

    def pack_side(values, lane):
        total = None
        for c, value in enumerate(values):
            spread = jnp.broadcast_to(value[:, :, lane : lane + 1], shape)
            chosen = jnp.where(lane3 == slot3 + 8 * c, spread, 0.0)
            flat = chosen[0] + chosen[1] + chosen[2] + chosen[3]
            part = flat[0:8] + flat[8:16]
            total = part if total is None else total + part
        return total

    def remote(e, k, src, dst, where_to):
        copy = pltpu.make_async_remote_copy(
            src_ref=src,
            dst_ref=dst,
            send_sem=halo_send_sem.at[e, k],
            recv_sem=halo_recv_sem.at[e, k],
            device_id=where_to,
            device_id_type=MESH,
        )
        copy.start()
        return copy

    def start_halo(e, buf, values, groups):
        edge = edge_recv.at[e] if len(values) <= 3 else basis_edge
        copies = [
            remote(e, 0, buf.at[:, 4, 8:24, :], buf.at[:, 0, 8:24, :], (gx_up, gy, gz)),
            remote(e, 1, buf.at[:, 1, 8:24, :], buf.at[:, 5, 8:24, :], (gx_dn, gy, gz)),
        ]
        pack_send[e, 0] = pack_side(values, LANES - 1)
        pack_send[e, 1] = pack_side(values, 0)
        copies.append(
            remote(e, 2, pack_send.at[e, 0], pack_recv.at[e, 0], (gx, gy, gz_up))
        )
        copies.append(
            remote(e, 3, pack_send.at[e, 1], pack_recv.at[e, 1], (gx, gy, gz_dn))
        )
        if groups is not None:
            copies.append(
                remote(e, 4, pack_send.at[e, 0], pack_recv.at[e, 2], (gx_dn, gy, gz_up))
            )
            copies.append(
                remote(e, 5, pack_send.at[e, 1], pack_recv.at[e, 3], (gx_up, gy, gz_dn))
            )
            copies.append(
                remote(
                    e, 6, pack_send.at[e, 1 - gy], pack_recv.at[e, 4], (gx, gy_other, gz_side)
                )
            )
            copies.append(
                remote(
                    e,
                    7,
                    buf.at[
                        pl.ds(len(groups[0]) * gy, len(groups[0])),
                        1 + 3 * gy,
                        pl.ds(pl.multiple_of(16 - 8 * gy, 8), 8),
                        :,
                    ],
                    edge,
                    (gx_side, gy_other, gz),
                )
            )
        copies.append(
            remote(
                e,
                8,
                buf.at[:, 1:5, pl.ds(pl.multiple_of(16 - 8 * gy, 8), 8), :],
                buf.at[:, 1:5, pl.ds(pl.multiple_of(24 * gy, 8), 8), :],
                (gx, gy_other, gz),
            )
        )
        return copies

    def finish_halo(e, buf, low_to, high_to, copies, groups):
        for copy in copies:
            copy.wait()
        count = buf.shape[0]
        for c in range(count):
            buf[c, 0, 8:24, :] = buf[c, 0, 8:24, :] * has_xm
            buf[c, 5, 8:24, :] = buf[c, 5, 8:24, :] * has_xp

        def spread_to(target, c, x, rows, pack, j):
            target[c, x, rows, :] = jnp.broadcast_to(pack[:, j : j + 1], (8, LANES))

        low = pack_recv[e, 0] * has_zm
        high = pack_recv[e, 1] * has_zp
        tiles = [slice(8, 16), slice(16, 24)]
        for c in range(count):
            for x in range(4):
                for t in range(2):
                    spread_to(low_to, c, 1 + x, tiles[t], low, 8 * c + 2 * x + t)
                    spread_to(high_to, c, 1 + x, tiles[t], high, 8 * c + 2 * x + t)
        if groups is not None:
            of_x, of_y, of_z = groups
            low_x = pack_recv[e, 2] * (has_xp * has_zm)
            high_x = pack_recv[e, 3] * (has_xm * has_zp)
            side = pack_recv[e, 4]
            low_y = side * (is_y0 * has_zm)
            high_y = side * (is_y1 * has_zp)
            for t in range(2):
                for c in of_x:
                    spread_to(low_to, c, 5, tiles[t], low_x, 8 * c + t)
                for c in of_z:
                    spread_to(high_to, c, 0, tiles[t], high_x, 8 * c + 6 + t)
            for x in range(4):
                for c in of_y:
                    spread_to(low_to, c, 1 + x, slice(24, 32), low_y, 8 * c + 2 * x)
                for c in of_z:
                    spread_to(high_to, c, 1 + x, slice(0, 8), high_y, 8 * c + 2 * x + 1)
            edge = edge_recv.at[e] if count <= 3 else basis_edge
            for k, c in enumerate(of_y):
                buf[c, 0, 24:32, :] = edge[k] * (is_y0 * has_xm)
            for k, c in enumerate(of_x):
                buf[c, 5, 0:8, :] = edge[k] * (is_y1 * has_xp)

    def before(value, low):
        return jnp.where(first_lane, low, pltpu.roll(value, 1, 2))

    def after(value, high):
        return jnp.where(last_lane, high, pltpu.roll(value, LANES - 1, 2))

    def set_field(e, values):
        for c in range(3):
            fields[e, c, 1:5, 8:24, :] = values[c]

    def stiffness(e):
        buf, low_z, high_z = (fields.at[e], low_all.at[e], high_all.at[e])
        u_z = buf[2, 0:5, 0:24, :]
        up_z = jnp.where(wide_lane, high_z[2, 0:5, 0:24, :], pltpu.roll(u_z, LANES - 1, 2))
        spread = (
            (buf[0, 1:6, 0:24, :] - buf[0, 0:5, 0:24, :])
            + (buf[1, 0:5, 1:25, :] - buf[1, 0:5, 0:24, :])
            + (up_z - u_z)
        )
        stress[...] = mod_buf[0, 0:5, 0:24, :] * spread
        here = stress[1:5, 8:24, :]
        spread_low = (
            (low_z[0, 2:6, 8:24, :] - low_z[0, 1:5, 8:24, :])
            + (low_z[1, 1:5, 9:25, :] - low_z[1, 1:5, 8:24, :])
            + (buf[2, 1:5, 8:24, :] - low_z[2, 1:5, 8:24, :])
        )
        below = [
            stress[0:4, 8:24, :],
            stress[1:5, 7:23, :],
            before(here, mod_low[0, 1:5, 8:24, :] * spread_low),
        ]
        images = []
        for c in range(3):
            centre = buf[c, 1:5, 8:24, :]
            image = coef[6] * centre
            image = image - coef[0] * buf[c, 0:4, 8:24, :]
            image = image - coef[1] * buf[c, 2:6, 8:24, :]
            image = image - coef[2] * buf[c, 1:5, 7:23, :]
            image = image - coef[3] * buf[c, 1:5, 9:25, :]
            image = image - coef[4] * before(centre, low_z[c, 1:5, 8:24, :])
            image = image - coef[5] * after(centre, high_z[c, 1:5, 8:24, :])
            images.append(image + LAME * (below[c] - here))
        return images

    def put_sum(q, value):
        if value.ndim == 3:
            value = value[0] + value[1] + value[2] + value[3]
        value = value[0:8] + value[8:16]
        rows_buf[q : q + 1, :] = jnp.sum(value, axis=0, keepdims=True)

    def make_row():
        sums = jnp.sum(rows_buf[...], axis=1, keepdims=True)
        return jnp.sum(jnp.where(diag2, sums, 0.0), axis=0, keepdims=True)

    me_group = gy * n_gz + gz

    def far_first(step):
        return wrap(step + n_gx // 2, n_gx - 1) + 1

    def rows_begin(i, row):
        row_send[i, 0] = row
        group_recv[i, me_group] = row

        def group_copy(step):
            return pltpu.make_async_remote_copy(
                src_ref=row_send.at[i, 0],
                dst_ref=group_recv.at[i, me_group],
                send_sem=row_send_sem.at[i, 0],
                recv_sem=row_recv_sem.at[i, 0],
                device_id=group_member(step),
                device_id_type=MESH,
            )

        def start_group(step, carry):
            group_copy(step).start()
            return carry

        lax.fori_loop(1, n_group, start_group, 0, unroll=True)

    def rows_middle(i):
        most = group_recv.at[i, pl.ds(0, n_group - 1)]
        pltpu.make_async_copy(most, most, row_recv_sem.at[i, 0]).wait()
        total = group_recv[i, 0]
        for k in range(1, n_group):
            total = total + group_recv[i, k]
        row_send[i, 1] = total
        slab_recv[i, gx] = total

        def start_slab(step, carry):
            pltpu.make_async_remote_copy(
                src_ref=row_send.at[i, 1],
                dst_ref=slab_recv.at[i, gx],
                send_sem=row_send_sem.at[i, 1],
                recv_sem=row_recv_sem.at[i, 1],
                device_id=(wrap(gx + far_first(step), n_gx), gy, gz),
                device_id_type=MESH,
            ).start()
            return carry

        lax.fori_loop(0, n_gx - 1, start_slab, 0, unroll=True)

    def rows_end(i):
        most = group_recv.at[i, pl.ds(0, n_group - 1)]
        rest = slab_recv.at[i, pl.ds(0, n_gx - 1)]
        pltpu.make_async_copy(rest, rest, row_recv_sem.at[i, 1]).wait()
        pltpu.make_async_copy(most, most, row_send_sem.at[i, 0]).wait()
        pltpu.make_async_copy(rest, rest, row_send_sem.at[i, 1]).wait()

    def slab_rows(i):
        table = jnp.concatenate(
            [slab_recv[i, k] for k in range(n_gx)]
            + [jnp.zeros((LANES - n_gx, LANES), F32)],
            axis=0,
        )
        return jnp.transpose(table)

    lane_row = lax.broadcasted_iota(jnp.int32, (1, LANES), 1)
    sub8 = lax.broadcasted_iota(jnp.int32, (8, LANES), 0)
    n_steps = steps_for(n_gx)

    def stack3(a, b, c):
        return jnp.where(sub8 == 0, a, jnp.where(sub8 == 1, b, jnp.where(sub8 == 2, c, 0.0)))

    def times(matrix, column):
        return (
            matrix[0] * column[0:1, :] + matrix[1] * column[1:2, :] + matrix[2] * column[2:3, :]
        )

    def inverse(cols):
        a, d, g = (cols[0][0:1, :], cols[0][1:2, :], cols[0][2:3, :])
        b, e, h = (cols[1][0:1, :], cols[1][1:2, :], cols[1][2:3, :])
        c, f, i = (cols[2][0:1, :], cols[2][1:2, :], cols[2][2:3, :])
        m00, m01, m02 = (e * i - f * h, c * h - b * i, b * f - c * e)
        m10, m11, m12 = (f * g - d * i, a * i - c * g, c * d - a * f)
        m20, m21, m22 = (d * h - e * g, b * g - a * h, a * e - b * d)
        scale = 1.0 / (a * m00 + b * m10 + c * m20)
        return [
            stack3(m00 * scale, m10 * scale, m20 * scale),
            stack3(m01 * scale, m11 * scale, m21 * scale),
            stack3(m02 * scale, m12 * scale, m22 * scale),
        ]

    def factorise(lower, main, upper, rhs):
        def body(step, carry):
            stride, low, mid, high, vec = carry
            back = LANES - stride
            inv = inverse(mid)
            inv_dn = [pltpu.roll(v, stride, 1) for v in inv]
            inv_up = [pltpu.roll(v, back, 1) for v in inv]
            alpha = [-times(low, v) for v in inv_dn]
            gamma = [-times(high, v) for v in inv_up]
            for k in range(3):
                pcr_buf[step, k] = alpha[k]
                pcr_buf[step, 3 + k] = gamma[k]
            low_dn = [pltpu.roll(v, stride, 1) for v in low]
            high_dn = [pltpu.roll(v, stride, 1) for v in high]
            low_up = [pltpu.roll(v, back, 1) for v in low]
            high_up = [pltpu.roll(v, back, 1) for v in high]
            vec_dn = pltpu.roll(vec, stride, 1)
            vec_up = pltpu.roll(vec, back, 1)
            new_mid = [
                mid[k] + times(alpha, high_dn[k]) + times(gamma, low_up[k]) for k in range(3)
            ]
            new_low = [times(alpha, v) for v in low_dn]
            new_high = [times(gamma, v) for v in high_up]
            new_vec = vec + times(alpha, vec_dn) + times(gamma, vec_up)
            return (stride * 2, new_low, new_mid, new_high, new_vec)

        _, _, mid, _, vec = lax.fori_loop(
            0, n_steps, body, (jnp.int32(1), lower, main, upper, rhs)
        )
        inv = inverse(mid)
        for k in range(3):
            pcr_buf[n_steps, k] = inv[k]
        return times(inv, vec)

    def solve_again(vec):
        stride = 1
        for step in range(n_steps):
            alpha = [pcr_buf[step, k] for k in range(3)]
            gamma = [pcr_buf[step, 3 + k] for k in range(3)]
            vec_dn = pltpu.roll(vec, stride, 1)
            vec_up = pltpu.roll(vec, LANES - stride, 1)
            vec = vec + times(alpha, vec_dn) + times(gamma, vec_up)
            stride *= 2
        return times([pcr_buf[n_steps, k] for k in range(3)], vec)

    def nearby(solved):
        turned = pltpu.roll(solved, wrap(1 - gx, LANES), 1)
        return [
            [jnp.broadcast_to(turned[c : c + 1, b : b + 1], (32, LANES)) for c in range(3)]
            for b in range(3)
        ]

    pl.semaphore_wait(barrier, len(near))

    plain = ((0,), (1,), (2,))
    copies = start_halo(0, mod_buf, [mod], None)
    flood(0, 4)
    finish_halo(0, mod_buf, mod_low, mod_high, copies, None)
    mod_zm = before(mod, mod_low[0, 1:5, 8:24, :])
    mod_zp = after(mod, mod_high[0, 1:5, 8:24, :])
    mod_xm, mod_xp = (mod_buf[0, 0:4, 8:24, :], mod_buf[0, 2:6, 8:24, :])
    mod_ym, mod_yp = (mod_buf[0, 1:5, 7:23, :], mod_buf[0, 1:5, 9:25, :])
    couplings = [0.5 * (mod + v) for v in (mod_xm, mod_xp, mod_ym, mod_yp, mod_zm, mod_zp)]
    total = fixed4
    for k in range(6):
        coef[k] = couplings[k]
        total = total + couplings[k]
    coef[6] = total
    for c in range(3):
        dinv_buf[c] = OMEGA / (total + couplings[2 * c])

    first = [load[c] * dinv_buf[c] for c in range(3)]
    set_field(0, first)
    copies = start_halo(1, fields.at[0], first, plain)
    flood(4, len(floods))

    low_y_edge = jnp.where(y3 == 0, is_y0, 0.0)
    high_y_edge = jnp.where(y3 == 15, is_y1, 0.0)
    low_z_edge = jnp.where(first_lane, 1.0 - has_zm, 0.0)
    high_z_edge = jnp.where(last_lane, 1.0 - has_zp, 0.0)
    first_x = jnp.where(x3 == 0, 1.0, 0.0)
    last_x = jnp.where(x3 == 3, 1.0, 0.0)
    bound = (
        fixed4
        + couplings[2] * low_y_edge
        + couplings[3] * high_y_edge
        + couplings[4] * low_z_edge
        + couplings[5] * high_z_edge
        + couplings[0] * first_x
        + couplings[1] * last_x
    )
    half = LAME * mod
    half_xm = LAME * mod_xm
    rows_buf[...] = jnp.zeros((16, LANES), F32)
    put_sum(0, bound + half_xm * first_x + half * last_x)
    put_sum(1, bound + half * high_y_edge)
    put_sum(2, bound + half * high_z_edge)
    put_sum(3, half[3] * high_y_edge[3])
    put_sum(4, half[3] * high_z_edge[3])
    put_sum(5, half * high_y_edge * high_z_edge)
    put_sum(6, couplings[1][3])
    put_sum(7, couplings[1][3] + half[3])

    dinv = [dinv_buf[c] for c in range(3)]
    inner_xm = half_xm * (1.0 - first_x)
    pieces = [
        dinv[0] * (bound + half_xm * first_x + half * last_x),
        dinv[0] * (half - inner_xm),
        dinv[0] * (first_x * (couplings[0] + half_xm) + last_x * (couplings[1] + half)),
        dinv[0] * first_x * half_xm,
        dinv[1] * (bound + half * high_y_edge),
        dinv[1] * (half - LAME * mod_ym),
        dinv[1] * (first_x * couplings[0] + last_x * couplings[1]),
        dinv[2] * (bound + half * high_z_edge),
        dinv[2] * (half - LAME * mod_zm),
        dinv[2] * (first_x * couplings[0] + last_x * couplings[1]),
    ]
    for c in range(N_BASIS):
        basis[c, 1:5, 8:24, :] = pieces[c]
    basis_groups = ((0, 1, 2, 3), (4, 5, 6), (7, 8, 9))

    whole = (6, 32, LANES)
    x6 = lax.broadcasted_iota(jnp.int32, whole, 0)
    y6 = lax.broadcasted_iota(jnp.int32, whole, 1)
    lane6 = lax.broadcasted_iota(jnp.int32, whole, 2)

    def coarse_fields(near):
        under, here, over = near
        inside = jnp.where(y6 < 8, is_y1, jnp.where(y6 >= 24, is_y0, 1.0))
        top_y = jnp.where(y6 == 23, is_y1, 0.0)
        top_z = jnp.where(lane6 == LANES - 1, 1.0 - has_zp, 0.0)
        own = [jnp.where(x6 == 0, under[c], jnp.where(x6 == 5, over[c], here[c])) for c in range(3)]
        other = [
            jnp.where(
                x6 == 1,
                under[c],
                jnp.where(
                    x6 == 4, over[c], jnp.where(jnp.logical_or(x6 == 0, x6 == 5), here[c], 0.0)
                ),
            )
            for c in range(3)
        ]
        drop = jnp.where(x6 == 4, here[0] - over[0], jnp.where(x6 == 0, under[0] - here[0], 0.0))
        own_y, other_y = (top_y * own[1], top_y * other[1])
        own_z, other_z = (top_z * own[2], top_z * other[2])

        def evaluate(b, scale, with_z):
            t_own = own_y + own_z if with_z else own_y
            t_other = other_y + other_z if with_z else other_y
            drop_y = drop + own_z if with_z else drop
            held = inside if scale is None else inside * scale
            return [
                (held - b[0]) * own[0] - b[1] * t_own + b[2] * other[0] + b[3] * t_other,
                (held - b[4]) * own[1] - b[5] * drop_y + b[6] * other[1],
                (held - b[7]) * own[2] - b[8] * (drop + own_y) + b[9] * other[2],
            ]

        return (
            evaluate(basis, None, True),
            evaluate(basis_low, has_zm, False),
            evaluate(basis_high, has_zp, False),
        )

    finish_halo(1, fields.at[0], low_all.at[0], high_all.at[0], copies, plain)
    image_first = stiffness(0)
    rest = [load[c] - image_first[c] for c in range(3)]
    for c in range(3):
        put_sum(8 + c, rest[c])
    rows_begin(0, make_row())
    partial = [first[c] + dinv_buf[c] * rest[c] for c in range(3)]
    set_field(1, partial)
    copies = start_halo(2, fields.at[1], partial, plain)
    more = start_halo(3, basis, [basis[c, 1:5, 8:24, :] for c in range(N_BASIS)], basis_groups)
    rows_middle(0)
    finish_halo(2, fields.at[1], low_all.at[1], high_all.at[1], copies, plain)
    finish_halo(3, basis, basis_low, basis_high, more, basis_groups)
    rows_end(0)

    table = slab_rows(0)
    real = lane_row < n_gx
    row = [jnp.where(real, table[q : q + 1, :], 0.0) for q in range(11)]
    one = jnp.where(real, 0.0, 1.0)
    none = jnp.zeros((1, LANES), F32)
    main = [
        stack3(row[0] + one, row[3], row[4]),
        stack3(row[3], row[1] + one, row[5]),
        stack3(row[4], row[5], row[2] + one),
    ]
    joined = lane_row < n_gx - 1
    side = [jnp.where(joined, row[q], 0.0) for q in (7, 3, 4, 6)]
    upper = [
        stack3(-side[0], -side[1], -side[2]),
        stack3(none, -side[3], none),
        stack3(none, none, -side[3]),
    ]
    moved = [pltpu.roll(jnp.broadcast_to(v, (8, LANES)), 1, 1)[0:1, :] for v in side]
    lower = [
        stack3(-moved[0], none, none),
        stack3(-moved[1], -moved[3], none),
        stack3(-moved[2], none, -moved[3]),
    ]
    near = nearby(factorise(lower, main, upper, stack3(row[8], row[9], row[10])))
    for target, extra in zip((fields, low_all, high_all), coarse_fields(near)):
        for c in range(3):
            target[1, c] = target[1, c] + extra[c]
    image = stiffness(1)
    smooth = []
    for c in range(3):
        keep[c] = image[c]
        smooth.append(dinv_buf[c] * image[c])
    set_field(2, smooth)
    copies = start_halo(4, fields.at[2], smooth, plain)
    rows_buf[...] = jnp.zeros((16, LANES), F32)
    precond = [fields[1, c, 1:5, 8:24, :] for c in range(3)]
    load = [in_forces[c] * load_scale for c in range(3)]
    put_sum(0, load[0] * precond[0] + load[1] * precond[1] + load[2] * precond[2])
    put_sum(1, image[0] * precond[0] + image[1] * precond[1] + image[2] * precond[2])
    finish_halo(4, fields.at[2], low_all.at[2], high_all.at[2], copies, plain)
    image_smooth = stiffness(2)
    change = []
    for c in range(3):
        remain = keep[c] - image_smooth[c]
        put_sum(2 + c, remain)
        change.append(fields[2, c, 1:5, 8:24, :] + dinv_buf[c] * remain)
    rows_begin(1, make_row())
    set_field(3, change)
    copies = start_halo(5, fields.at[3], change, plain)
    rows_middle(1)
    finish_halo(5, fields.at[3], low_all.at[3], high_all.at[3], copies, plain)
    rows_end(1)

    table = slab_rows(1)
    row = [jnp.where(real, table[q : q + 1, :], 0.0) for q in range(5)]
    norm_now = jnp.sum(row[0], axis=1, keepdims=True)
    curve = jnp.sum(row[1], axis=1, keepdims=True)
    step0 = norm_now / curve
    near = nearby(solve_again(stack3(row[2], row[3], row[4])))
    wide0 = jnp.broadcast_to(step0, (32, LANES))
    for target, extra in zip((fields, low_all, high_all), coarse_fields(near)):
        for c in range(3):
            target[3, c] = target[1, c] - wide0 * (target[3, c] + extra[c])
    wide0 = jnp.broadcast_to(step0, (16, LANES))
    image_next = stiffness(3)
    rows_buf[...] = jnp.zeros((16, LANES), F32)
    norm_part = jnp.zeros(shape, F32)
    curve_part = jnp.zeros(shape, F32)
    for c in range(3):
        following = fields[3, c, 1:5, 8:24, :]
        residual = in_forces[c] * load_scale - wide0 * keep[c]
        norm_part = norm_part + residual * following
        curve_part = curve_part + image_next[c] * following
        keep[3 + c] = residual
        keep[6 + c] = image_next[c]
    put_sum(0, norm_part)
    put_sum(1, curve_part)
    rows_begin(2, make_row())
    rows_middle(2)
    rows_end(2)

    both = slab_recv[2, 0]
    for k in range(1, n_gx):
        both = both + slab_recv[2, k]
    norm_next, curve_next = (both[0:1, 0:1], both[0:1, 1:2])
    ratio = norm_next / norm_now
    step1 = norm_next / (curve_next - ratio * norm_next / step0)
    wide_ratio = jnp.broadcast_to(ratio, (16, LANES))
    wide1 = jnp.broadcast_to(step1, (16, LANES))
    for c in range(3):
        previous = fields[1, c, 1:5, 8:24, :]
        search = fields[3, c, 1:5, 8:24, :] + wide_ratio * previous
        disp_out[c] = wide0 * previous + wide1 * search
        res_out[c] = keep[3 + c] - wide1 * (keep[6 + c] + wide_ratio * keep[c])


def solution(mesh):
    sizes = tuple(mesh.shape[name] for name in ("gx", "gy", "gz"))
    n_gx, n_gy, n_gz = sizes
    n_group = n_gy * n_gz
    block = jax.ShapeDtypeStruct((3, 4, 16, LANES), F32)
    vmem = pl.BlockSpec(memory_space=pltpu.VMEM)

    def body(density, fixed_mask, load_mask, forces):
        def run(*refs):
            kernel(sizes, *refs)

        return pl.pallas_call(
            run,
            out_shape=(block, block),
            in_specs=[pl.BlockSpec(memory_space=pl.ANY)] * 4,
            out_specs=(vmem, vmem),
            scratch_shapes=[
                pltpu.VMEM((1, 6, 32, LANES), F32),
                pltpu.VMEM((N_FIELD, 3, 6, 32, LANES), F32),
                pltpu.VMEM((N_FIELD, 3, 6, 32, LANES), F32),
                pltpu.VMEM((N_FIELD, 3, 6, 32, LANES), F32),
                pltpu.VMEM((1, 6, 32, LANES), F32),
                pltpu.VMEM((1, 6, 32, LANES), F32),
                pltpu.VMEM((N_BASIS, 6, 32, LANES), F32),
                pltpu.VMEM((N_BASIS, 6, 32, LANES), F32),
                pltpu.VMEM((N_BASIS, 6, 32, LANES), F32),
                pltpu.VMEM((N_EX, 2, 8, LANES), F32),
                pltpu.VMEM((N_EX, 5, 8, LANES), F32),
                pltpu.VMEM((N_EX, 1, 8, LANES), F32),
                pltpu.VMEM((4, 8, LANES), F32),
                pltpu.VMEM((5, 24, LANES), F32),
                pltpu.VMEM((7, 4, 16, LANES), F32),
                pltpu.VMEM((3, 4, 16, LANES), F32),
                pltpu.VMEM((9, 4, 16, LANES), F32),
                pltpu.VMEM((16, LANES), F32),
                pltpu.VMEM((steps_for(n_gx) + 1, 6, 8, LANES), F32),
                pltpu.VMEM((3, 2, 1, LANES), F32),
                pltpu.VMEM((3, n_group, 1, LANES), F32),
                pltpu.VMEM((3, n_gx, 1, LANES), F32),
                pltpu.VMEM((4, 16, LANES), jnp.int32),
                pltpu.VMEM((4, 16, LANES), jnp.int32),
                pltpu.VMEM((4, 16, LANES), jnp.int32),
                pltpu.VMEM((3, 4, 16, LANES), F32),
                pltpu.SemaphoreType.DMA((4,)),
                pltpu.SemaphoreType.DMA((N_EX, N_MSG)),
                pltpu.SemaphoreType.DMA((N_EX, N_MSG)),
                pltpu.SemaphoreType.DMA((3, 2)),
                pltpu.SemaphoreType.DMA((3, 2)),
                pltpu.SemaphoreType.REGULAR((8, 2)),
            ],
            compiler_params=pltpu.CompilerParams(collective_id=0, has_side_effects=True),
        )(density, fixed_mask, load_mask, forces)

    spec = P("gx", "gy", "gz")
    wide = P(None, "gx", "gy", "gz")
    return jax.shard_map(
        body,
        mesh=mesh,
        in_specs=(spec, spec, spec, wide),
        out_specs=(wide, wide),
        check_vma=False,
    )
```

```python
import jax
import jax.numpy as jnp
from jax import lax
from jax.experimental import pallas as pl
from jax.experimental.pallas import tpu as pltpu
from jax.sharding import PartitionSpec as P

LAME = 0.5
PENALTY = 4.0
OMEGA = 0.5
F32 = jnp.float32
MESH = pl.DeviceIdType.MESH
LANES = 128
N_MSG = 9
N_EX = 6
N_FIELD = 5
N_ROWS = 104
FIRST_G = 16
N_BASIS = 10


def steps_for(count):
    steps = 0
    while (1 << steps) < count:
        steps += 1
    return steps


def kernel(
    sizes,
    density,
    fixed_mask,
    load_mask,
    forces,
    disp_out,
    res_out,
    mod_buf,
    fields,
    low_all,
    high_all,
    mod_low,
    mod_high,
    basis,
    basis_low,
    basis_high,
    pack_send,
    pack_recv,
    edge_recv,
    basis_edge,
    stress,
    coef,
    dinv_buf,
    keep,
    rows_buf,
    units,
    pcr_buf,
    row_send,
    group_recv,
    slab_recv,
    in_density,
    in_fixed,
    in_load,
    in_forces,
    in_sem,
    halo_send_sem,
    halo_recv_sem,
    row_send_sem,
    row_recv_sem,
    flood_sem,
):
    n_gx, n_gy, n_gz = sizes
    n_group = n_gy * n_gz
    gx, gy, gz = (lax.axis_index("gx"), lax.axis_index("gy"), lax.axis_index("gz"))

    def wrap(value, count):
        value = jnp.where(value >= count, value - count, value)
        return jnp.where(value < 0, value + count, value)

    gx_up, gx_dn = (wrap(gx + 1, n_gx), wrap(gx - 1, n_gx))
    gz_up, gz_dn = (wrap(gz + 1, n_gz), wrap(gz - 1, n_gz))
    gy_other = 1 - gy
    gx_side = wrap(gx + 2 * gy - 1, n_gx)
    gz_side = wrap(gz + 2 * gy - 1, n_gz)

    def group_member(step):
        y_at = jnp.where(step >= n_gz, gy_other, gy)
        z_at = wrap(gz + jnp.where(step >= n_gz, step - n_gz, step), n_gz)
        return (gx, y_at, z_at)

    barrier = pltpu.get_barrier_semaphore()

    def greet(where_to):
        pl.semaphore_signal(barrier, inc=1, device_id=where_to, device_id_type=MESH)

    near = [
        (gx_up, gy, gz),
        (gx_dn, gy, gz),
        (gx, gy, gz_up),
        (gx, gy, gz_dn),
        (gx, gy_other, gz),
        (gx_side, gy_other, gz),
        (gx_dn, gy, gz_up),
        (gx_up, gy, gz_dn),
        (gx, gy_other, gz_side),
    ]
    n_fast = 12 if n_gx == 48 else n_gx
    n_slow = n_gx // n_fast
    slow = gx // n_fast
    fast = gx - slow * n_fast
    ring_fast = [slow * n_fast + wrap(fast + d, n_fast) for d in (1, -1)]
    ring_slow = [wrap(slow + d, n_slow) * n_fast + fast for d in (1, -1)]
    if n_slow > 1:
        near = near + [(v, gy, gz) for v in ring_slow + ring_fast]
    for where_to in near:
        greet(where_to)
    fetches = []
    for k, (src, dst) in enumerate(
        ((density, in_density), (fixed_mask, in_fixed), (load_mask, in_load), (forces, in_forces))
    ):
        fetch = pltpu.make_async_copy(src, dst, in_sem.at[k])
        fetch.start()
        fetches.append(fetch)

    ring_y = [(gx, gy, gz_up), (gx, gy, gz_dn)]
    ring_z = [(v, gy, gz) for v in ring_fast]
    ring_x = [(v, gy, gz) for v in ring_slow]
    n_y, n_z = (max(n_gz // 2 - 1, 0), max(n_fast // 2 - 1, 0))
    floods = []
    for k in range(max(n_y, n_z)):
        floods.append(([ring_y] if k < n_y else []) + ([ring_z] if k < n_z else []))
    if n_slow > 1:
        floods += [[ring_x]] * max(n_slow // 2, 1)

    def flood(first, last):
        for k in range(first, min(last, len(floods))):
            for r, ring in enumerate(floods[k]):
                for where_to in ring:
                    pl.semaphore_signal(
                        flood_sem.at[k, r], inc=1, device_id=where_to, device_id_type=MESH
                    )
            for r in range(len(floods[k])):
                pl.semaphore_wait(flood_sem.at[k, r], 2)

    has_xm = jnp.where(gx > 0, 1.0, 0.0).astype(F32)
    has_xp = jnp.where(gx < n_gx - 1, 1.0, 0.0).astype(F32)
    has_zm = jnp.where(gz > 0, 1.0, 0.0).astype(F32)
    has_zp = jnp.where(gz < n_gz - 1, 1.0, 0.0).astype(F32)
    is_y0 = jnp.where(gy == 0, 1.0, 0.0).astype(F32)
    is_y1 = 1.0 - is_y0

    shape = (4, 16, LANES)
    lane3 = lax.broadcasted_iota(jnp.int32, shape, 2)
    x3 = lax.broadcasted_iota(jnp.int32, shape, 0)
    y3 = lax.broadcasted_iota(jnp.int32, shape, 1)
    slot3 = 2 * x3 + jnp.where(y3 >= 8, 1, 0)
    first_lane, last_lane = (lane3 == 0, lane3 == LANES - 1)
    wide_lane = lax.broadcasted_iota(jnp.int32, (5, 24, LANES), 2) == LANES - 1
    table_shape = (N_ROWS, LANES)
    diag2 = lax.broadcasted_iota(jnp.int32, table_shape, 1) == lax.broadcasted_iota(
        jnp.int32, table_shape, 0
    )

    zeros_side = jnp.zeros((4, 8, LANES), F32)
    outside = pl.ds(pl.multiple_of(24 * gy, 8), 8)
    padded = [(mod_buf, 1), (basis, N_BASIS)] + [(fields.at[e], 3) for e in range(4)]
    for buf, count in padded:
        for c in range(count):
            buf[c, 1:5, outside, :] = zeros_side

    for fetch in fetches:
        fetch.wait()
    level = in_density[...].astype(F32) / 15.0
    mod = 0.05 + 0.95 * level * level * level
    mod_buf[0, 1:5, 8:24, :] = mod
    fixed4 = PENALTY * in_fixed[...].astype(F32)
    load_scale = 0.25 + in_load[...].astype(F32)
    load = [in_forces[c] * load_scale for c in range(3)]

    def pack_side(values, lane):
        total = None
        for c, value in enumerate(values):
            spread = jnp.broadcast_to(value[:, :, lane : lane + 1], shape)
            chosen = jnp.where(lane3 == slot3 + 8 * c, spread, 0.0)
            flat = chosen[0] + chosen[1] + chosen[2] + chosen[3]
            part = flat[0:8] + flat[8:16]
            total = part if total is None else total + part
        return total

    def remote(e, k, src, dst, where_to):
        copy = pltpu.make_async_remote_copy(
            src_ref=src,
            dst_ref=dst,
            send_sem=halo_send_sem.at[e, k],
            recv_sem=halo_recv_sem.at[e, k],
            device_id=where_to,
            device_id_type=MESH,
        )
        copy.start()
        return copy

    def start_halo(e, buf, values, groups):
        edge = edge_recv.at[e] if len(values) <= 3 else basis_edge
        copies = [
            remote(e, 0, buf.at[:, 4, 8:24, :], buf.at[:, 0, 8:24, :], (gx_up, gy, gz)),
            remote(e, 1, buf.at[:, 1, 8:24, :], buf.at[:, 5, 8:24, :], (gx_dn, gy, gz)),
        ]
        pack_send[e, 0] = pack_side(values, LANES - 1)
        pack_send[e, 1] = pack_side(values, 0)
        copies.append(
            remote(e, 2, pack_send.at[e, 0], pack_recv.at[e, 0], (gx, gy, gz_up))
        )
        copies.append(
            remote(e, 3, pack_send.at[e, 1], pack_recv.at[e, 1], (gx, gy, gz_dn))
        )
        if groups is not None:
            copies.append(
                remote(e, 4, pack_send.at[e, 0], pack_recv.at[e, 2], (gx_dn, gy, gz_up))
            )
            copies.append(
                remote(e, 5, pack_send.at[e, 1], pack_recv.at[e, 3], (gx_up, gy, gz_dn))
            )
            copies.append(
                remote(
                    e, 6, pack_send.at[e, 1 - gy], pack_recv.at[e, 4], (gx, gy_other, gz_side)
                )
            )
            copies.append(
                remote(
                    e,
                    7,
                    buf.at[
                        pl.ds(len(groups[0]) * gy, len(groups[0])),
                        1 + 3 * gy,
                        pl.ds(pl.multiple_of(16 - 8 * gy, 8), 8),
                        :,
                    ],
                    edge,
                    (gx_side, gy_other, gz),
                )
            )
        copies.append(
            remote(
                e,
                8,
                buf.at[:, 1:5, pl.ds(pl.multiple_of(16 - 8 * gy, 8), 8), :],
                buf.at[:, 1:5, pl.ds(pl.multiple_of(24 * gy, 8), 8), :],
                (gx, gy_other, gz),
            )
        )
        return copies

    def finish_halo(e, buf, low_to, high_to, copies, groups):
        for copy in copies:
            copy.wait()
        count = buf.shape[0]
        for c in range(count):
            buf[c, 0, 8:24, :] = buf[c, 0, 8:24, :] * has_xm
            buf[c, 5, 8:24, :] = buf[c, 5, 8:24, :] * has_xp

        def spread_to(target, c, x, rows, pack, j):
            target[c, x, rows, :] = jnp.broadcast_to(pack[:, j : j + 1], (8, LANES))

        low = pack_recv[e, 0] * has_zm
        high = pack_recv[e, 1] * has_zp
        tiles = [slice(8, 16), slice(16, 24)]
        for c in range(count):
            for x in range(4):
                for t in range(2):
                    spread_to(low_to, c, 1 + x, tiles[t], low, 8 * c + 2 * x + t)
                    spread_to(high_to, c, 1 + x, tiles[t], high, 8 * c + 2 * x + t)
        if groups is not None:
            of_x, of_y, of_z = groups
            low_x = pack_recv[e, 2] * (has_xp * has_zm)
            high_x = pack_recv[e, 3] * (has_xm * has_zp)
            side = pack_recv[e, 4]
            low_y = side * (is_y0 * has_zm)
            high_y = side * (is_y1 * has_zp)
            for t in range(2):
                for c in of_x:
                    spread_to(low_to, c, 5, tiles[t], low_x, 8 * c + t)
                for c in of_z:
                    spread_to(high_to, c, 0, tiles[t], high_x, 8 * c + 6 + t)
            for x in range(4):
                for c in of_y:
                    spread_to(low_to, c, 1 + x, slice(24, 32), low_y, 8 * c + 2 * x)
                for c in of_z:
                    spread_to(high_to, c, 1 + x, slice(0, 8), high_y, 8 * c + 2 * x + 1)
            edge = edge_recv.at[e] if count <= 3 else basis_edge
            for k, c in enumerate(of_y):
                buf[c, 0, 24:32, :] = edge[k] * (is_y0 * has_xm)
            for k, c in enumerate(of_x):
                buf[c, 5, 0:8, :] = edge[k] * (is_y1 * has_xp)

    def before(value, low):
        return jnp.where(first_lane, low, pltpu.roll(value, 1, 2))

    def after(value, high):
        return jnp.where(last_lane, high, pltpu.roll(value, LANES - 1, 2))

    def set_field(e, values):
        for c in range(3):
            fields[e, c, 1:5, 8:24, :] = values[c]

    def stiffness(e):
        buf, low_z, high_z = (fields.at[e], low_all.at[e], high_all.at[e])
        u_z = buf[2, 0:5, 0:24, :]
        up_z = jnp.where(wide_lane, high_z[2, 0:5, 0:24, :], pltpu.roll(u_z, LANES - 1, 2))
        spread = (
            (buf[0, 1:6, 0:24, :] - buf[0, 0:5, 0:24, :])
            + (buf[1, 0:5, 1:25, :] - buf[1, 0:5, 0:24, :])
            + (up_z - u_z)
        )
        stress[...] = mod_buf[0, 0:5, 0:24, :] * spread
        here = stress[1:5, 8:24, :]
        spread_low = (
            (low_z[0, 2:6, 8:24, :] - low_z[0, 1:5, 8:24, :])
            + (low_z[1, 1:5, 9:25, :] - low_z[1, 1:5, 8:24, :])
            + (buf[2, 1:5, 8:24, :] - low_z[2, 1:5, 8:24, :])
        )
        below = [
            stress[0:4, 8:24, :],
            stress[1:5, 7:23, :],
            before(here, mod_low[0, 1:5, 8:24, :] * spread_low),
        ]
        images = []
        for c in range(3):
            centre = buf[c, 1:5, 8:24, :]
            image = coef[6] * centre
            image = image - coef[0] * buf[c, 0:4, 8:24, :]
            image = image - coef[1] * buf[c, 2:6, 8:24, :]
            image = image - coef[2] * buf[c, 1:5, 7:23, :]
            image = image - coef[3] * buf[c, 1:5, 9:25, :]
            image = image - coef[4] * before(centre, low_z[c, 1:5, 8:24, :])
            image = image - coef[5] * after(centre, high_z[c, 1:5, 8:24, :])
            images.append(image + LAME * (below[c] - here))
        return images

    def put_sum(q, value):
        if value.ndim == 3:
            value = value[0] + value[1] + value[2] + value[3]
        value = value[0:8] + value[8:16]
        rows_buf[pl.ds(q, 1), :] = jnp.sum(value, axis=0, keepdims=True)

    def make_row():
        sums = jnp.sum(rows_buf[...], axis=1, keepdims=True)
        return jnp.sum(jnp.where(diag2, sums, 0.0), axis=0, keepdims=True)

    me_group = gy * n_gz + gz

    def far_first(step):
        return wrap(step + n_gx // 2, n_gx - 1) + 1

    def rows_begin(i, row):
        row_send[i, 0] = row
        group_recv[i, me_group] = row

        def group_copy(step):
            return pltpu.make_async_remote_copy(
                src_ref=row_send.at[i, 0],
                dst_ref=group_recv.at[i, me_group],
                send_sem=row_send_sem.at[i, 0],
                recv_sem=row_recv_sem.at[i, 0],
                device_id=group_member(step),
                device_id_type=MESH,
            )

        def start_group(step, carry):
            group_copy(step).start()
            return carry

        lax.fori_loop(1, n_group, start_group, 0, unroll=True)

    def rows_middle(i):
        most = group_recv.at[i, pl.ds(0, n_group - 1)]
        pltpu.make_async_copy(most, most, row_recv_sem.at[i, 0]).wait()
        total = group_recv[i, 0]
        for k in range(1, n_group):
            total = total + group_recv[i, k]
        row_send[i, 1] = total
        slab_recv[i, gx] = total

        def start_slab(step, carry):
            pltpu.make_async_remote_copy(
                src_ref=row_send.at[i, 1],
                dst_ref=slab_recv.at[i, gx],
                send_sem=row_send_sem.at[i, 1],
                recv_sem=row_recv_sem.at[i, 1],
                device_id=(wrap(gx + far_first(step), n_gx), gy, gz),
                device_id_type=MESH,
            ).start()
            return carry

        lax.fori_loop(0, n_gx - 1, start_slab, 0, unroll=True)

    def rows_end(i):
        most = group_recv.at[i, pl.ds(0, n_group - 1)]
        rest = slab_recv.at[i, pl.ds(0, n_gx - 1)]
        pltpu.make_async_copy(rest, rest, row_recv_sem.at[i, 1]).wait()
        pltpu.make_async_copy(most, most, row_send_sem.at[i, 0]).wait()
        pltpu.make_async_copy(rest, rest, row_send_sem.at[i, 1]).wait()

    def slab_rows(i):
        table = jnp.concatenate(
            [slab_recv[i, k] for k in range(n_gx)]
            + [jnp.zeros((LANES - n_gx, LANES), F32)],
            axis=0,
        )
        return jnp.transpose(table)

    lane_row = lax.broadcasted_iota(jnp.int32, (1, LANES), 1)
    sub8 = lax.broadcasted_iota(jnp.int32, (8, LANES), 0)
    n_steps = steps_for(n_gx)

    def stack3(a, b, c):
        return jnp.where(sub8 == 0, a, jnp.where(sub8 == 1, b, jnp.where(sub8 == 2, c, 0.0)))

    def times(matrix, column):
        return (
            matrix[0] * column[0:1, :] + matrix[1] * column[1:2, :] + matrix[2] * column[2:3, :]
        )

    def inverse(cols):
        a, d, g = (cols[0][0:1, :], cols[0][1:2, :], cols[0][2:3, :])
        b, e, h = (cols[1][0:1, :], cols[1][1:2, :], cols[1][2:3, :])
        c, f, i = (cols[2][0:1, :], cols[2][1:2, :], cols[2][2:3, :])
        m00, m01, m02 = (e * i - f * h, c * h - b * i, b * f - c * e)
        m10, m11, m12 = (f * g - d * i, a * i - c * g, c * d - a * f)
        m20, m21, m22 = (d * h - e * g, b * g - a * h, a * e - b * d)
        scale = 1.0 / (a * m00 + b * m10 + c * m20)
        return [
            stack3(m00 * scale, m10 * scale, m20 * scale),
            stack3(m01 * scale, m11 * scale, m21 * scale),
            stack3(m02 * scale, m12 * scale, m22 * scale),
        ]

    def factorise(lower, main, upper, rhs):
        def body(step, carry):
            stride, low, mid, high, vec = carry
            back = LANES - stride
            inv = inverse(mid)
            inv_dn = [pltpu.roll(v, stride, 1) for v in inv]
            inv_up = [pltpu.roll(v, back, 1) for v in inv]
            alpha = [-times(low, v) for v in inv_dn]
            gamma = [-times(high, v) for v in inv_up]
            for k in range(3):
                pcr_buf[step, k] = alpha[k]
                pcr_buf[step, 3 + k] = gamma[k]
            low_dn = [pltpu.roll(v, stride, 1) for v in low]
            high_dn = [pltpu.roll(v, stride, 1) for v in high]
            low_up = [pltpu.roll(v, back, 1) for v in low]
            high_up = [pltpu.roll(v, back, 1) for v in high]
            vec_dn = pltpu.roll(vec, stride, 1)
            vec_up = pltpu.roll(vec, back, 1)
            new_mid = [
                mid[k] + times(alpha, high_dn[k]) + times(gamma, low_up[k]) for k in range(3)
            ]
            new_low = [times(alpha, v) for v in low_dn]
            new_high = [times(gamma, v) for v in high_up]
            new_vec = vec + times(alpha, vec_dn) + times(gamma, vec_up)
            return (stride * 2, new_low, new_mid, new_high, new_vec)

        _, _, mid, _, vec = lax.fori_loop(
            0, n_steps, body, (jnp.int32(1), lower, main, upper, rhs)
        )
        inv = inverse(mid)
        for k in range(3):
            pcr_buf[n_steps, k] = inv[k]
        return times(inv, vec)

    def solve_again(vec):
        stride = 1
        for step in range(n_steps):
            alpha = [pcr_buf[step, k] for k in range(3)]
            gamma = [pcr_buf[step, 3 + k] for k in range(3)]
            vec_dn = pltpu.roll(vec, stride, 1)
            vec_up = pltpu.roll(vec, LANES - stride, 1)
            vec = vec + times(alpha, vec_dn) + times(gamma, vec_up)
            stride *= 2
        return times([pcr_buf[n_steps, k] for k in range(3)], vec)

    def nearby(solved):
        turned = pltpu.roll(solved, wrap(1 - gx, LANES), 1)
        return [
            [jnp.broadcast_to(turned[c : c + 1, b : b + 1], (32, LANES)) for c in range(3)]
            for b in range(3)
        ]

    pl.semaphore_wait(barrier, len(near))

    plain = ((0,), (1,), (2,))
    copies = start_halo(0, mod_buf, [mod], None)
    flood(0, 4)
    finish_halo(0, mod_buf, mod_low, mod_high, copies, None)
    mod_zm = before(mod, mod_low[0, 1:5, 8:24, :])
    mod_zp = after(mod, mod_high[0, 1:5, 8:24, :])
    mod_xm, mod_xp = (mod_buf[0, 0:4, 8:24, :], mod_buf[0, 2:6, 8:24, :])
    mod_ym, mod_yp = (mod_buf[0, 1:5, 7:23, :], mod_buf[0, 1:5, 9:25, :])
    couplings = [0.5 * (mod + v) for v in (mod_xm, mod_xp, mod_ym, mod_yp, mod_zm, mod_zp)]
    total = fixed4
    for k in range(6):
        coef[k] = couplings[k]
        total = total + couplings[k]
    coef[6] = total
    for c in range(3):
        dinv_buf[c] = OMEGA / (total + couplings[2 * c])

    first = [load[c] * dinv_buf[c] for c in range(3)]
    set_field(0, first)
    copies = start_halo(1, fields.at[0], first, plain)
    flood(4, len(floods))

    low_y_edge = jnp.where(y3 == 0, is_y0, 0.0)
    high_y_edge = jnp.where(y3 == 15, is_y1, 0.0)
    low_z_edge = jnp.where(first_lane, 1.0 - has_zm, 0.0)
    high_z_edge = jnp.where(last_lane, 1.0 - has_zp, 0.0)
    first_x = jnp.where(x3 == 0, 1.0, 0.0)
    last_x = jnp.where(x3 == 3, 1.0, 0.0)
    bound = (
        fixed4
        + couplings[2] * low_y_edge
        + couplings[3] * high_y_edge
        + couplings[4] * low_z_edge
        + couplings[5] * high_z_edge
        + couplings[0] * first_x
        + couplings[1] * last_x
    )
    half = LAME * mod
    half_xm = LAME * mod_xm
    rows_buf[...] = jnp.zeros(table_shape, F32)
    put_sum(0, bound + half_xm * first_x + half * last_x)
    put_sum(1, bound + half * high_y_edge)
    put_sum(2, bound + half * high_z_edge)
    put_sum(3, half[3] * high_y_edge[3])
    put_sum(4, half[3] * high_z_edge[3])
    put_sum(5, half * high_y_edge * high_z_edge)
    put_sum(6, couplings[1][3])
    put_sum(7, couplings[1][3] + half[3])

    dinv = [dinv_buf[c] for c in range(3)]
    inner_xm = half_xm * (1.0 - first_x)
    pieces = [
        dinv[0] * (bound + half_xm * first_x + half * last_x),
        dinv[0] * (half - inner_xm),
        dinv[0] * (first_x * (couplings[0] + half_xm) + last_x * (couplings[1] + half)),
        dinv[0] * first_x * half_xm,
        dinv[1] * (bound + half * high_y_edge),
        dinv[1] * (half - LAME * mod_ym),
        dinv[1] * (first_x * couplings[0] + last_x * couplings[1]),
        dinv[2] * (bound + half * high_z_edge),
        dinv[2] * (half - LAME * mod_zm),
        dinv[2] * (first_x * couplings[0] + last_x * couplings[1]),
    ]
    for c in range(N_BASIS):
        basis[c, 1:5, 8:24, :] = pieces[c]
    basis_groups = ((0, 1, 2, 3), (4, 5, 6), (7, 8, 9))

    whole = (6, 32, LANES)
    x6 = lax.broadcasted_iota(jnp.int32, whole, 0)
    y6 = lax.broadcasted_iota(jnp.int32, whole, 1)
    lane6 = lax.broadcasted_iota(jnp.int32, whole, 2)

    def coarse_fields(near):
        under, here, over = near
        inside = jnp.where(y6 < 8, is_y1, jnp.where(y6 >= 24, is_y0, 1.0))
        top_y = jnp.where(y6 == 23, is_y1, 0.0)
        top_z = jnp.where(lane6 == LANES - 1, 1.0 - has_zp, 0.0)
        own = [jnp.where(x6 == 0, under[c], jnp.where(x6 == 5, over[c], here[c])) for c in range(3)]
        other = [
            jnp.where(
                x6 == 1,
                under[c],
                jnp.where(
                    x6 == 4, over[c], jnp.where(jnp.logical_or(x6 == 0, x6 == 5), here[c], 0.0)
                ),
            )
            for c in range(3)
        ]
        drop = jnp.where(x6 == 4, here[0] - over[0], jnp.where(x6 == 0, under[0] - here[0], 0.0))
        own_y, other_y = (top_y * own[1], top_y * other[1])
        own_z, other_z = (top_z * own[2], top_z * other[2])

        def evaluate(b, scale, with_z):
            t_own = own_y + own_z if with_z else own_y
            t_other = other_y + other_z if with_z else other_y
            drop_y = drop + own_z if with_z else drop
            held = inside if scale is None else inside * scale
            return [
                (held - b[0]) * own[0] - b[1] * t_own + b[2] * other[0] + b[3] * t_other,
                (held - b[4]) * own[1] - b[5] * drop_y + b[6] * other[1],
                (held - b[7]) * own[2] - b[8] * (drop + own_y) + b[9] * other[2],
            ]

        return (
            evaluate(basis, None, True),
            evaluate(basis_low, has_zm, False),
            evaluate(basis_high, has_zp, False),
        )

    def dot3(left, right):
        return left[0] * right[0] + left[1] * right[1] + left[2] * right[2]

    def unit_products(first_unit, last_unit):
        def body(i, carry):
            near = [
                [
                    jnp.broadcast_to(jnp.where(i == 3 * b + c, 1.0, 0.0).astype(F32), (32, LANES))
                    for c in range(3)
                ]
                for b in range(3)
            ]
            for target, value in zip((fields, low_all, high_all), coarse_fields(near)):
                for c in range(3):
                    target[4, c] = value[c]
            for c in range(3):
                units[i, c] = fields[4, c, 1:5, 8:24, :]
            image = stiffness(4)
            for j in range(9):
                put_sum(FIRST_G + 9 * i + j, dot3(image, [units[j, c] for c in range(3)]))
            return carry

        lax.fori_loop(first_unit, last_unit, body, 0)

    units[...] = jnp.zeros((9, 3, 4, 16, LANES), F32)
    finish_halo(1, fields.at[0], low_all.at[0], high_all.at[0], copies, plain)
    image_first = stiffness(0)
    rest = [load[c] - image_first[c] for c in range(3)]
    for c in range(3):
        put_sum(8 + c, rest[c])
    rows_begin(0, make_row())
    partial = [first[c] + dinv_buf[c] * rest[c] for c in range(3)]
    set_field(1, partial)
    copies = start_halo(2, fields.at[1], partial, plain)
    more = start_halo(3, basis, [basis[c, 1:5, 8:24, :] for c in range(N_BASIS)], basis_groups)
    rows_middle(0)
    finish_halo(2, fields.at[1], low_all.at[1], high_all.at[1], copies, plain)
    finish_halo(3, basis, basis_low, basis_high, more, basis_groups)
    unit_products(0, 3)
    rows_end(0)

    table = slab_rows(0)
    real = lane_row < n_gx
    row = [jnp.where(real, table[q : q + 1, :], 0.0) for q in range(11)]
    one = jnp.where(real, 0.0, 1.0)
    none = jnp.zeros((1, LANES), F32)
    main = [
        stack3(row[0] + one, row[3], row[4]),
        stack3(row[3], row[1] + one, row[5]),
        stack3(row[4], row[5], row[2] + one),
    ]
    joined = lane_row < n_gx - 1
    side = [jnp.where(joined, row[q], 0.0) for q in (7, 3, 4, 6)]
    upper = [
        stack3(-side[0], -side[1], -side[2]),
        stack3(none, -side[3], none),
        stack3(none, none, -side[3]),
    ]
    moved = [pltpu.roll(jnp.broadcast_to(v, (8, LANES)), 1, 1)[0:1, :] for v in side]
    lower = [
        stack3(-moved[0], none, none),
        stack3(-moved[1], -moved[3], none),
        stack3(-moved[2], none, -moved[3]),
    ]
    near = nearby(factorise(lower, main, upper, stack3(row[8], row[9], row[10])))
    for target, extra in zip((fields, low_all, high_all), coarse_fields(near)):
        for c in range(3):
            target[1, c] = target[1, c] + extra[c]
    image = stiffness(1)
    smooth = []
    for c in range(3):
        keep[c] = image[c]
        smooth.append(dinv_buf[c] * image[c])
    set_field(2, smooth)
    copies = start_halo(4, fields.at[2], smooth, plain)
    precond = [fields[1, c, 1:5, 8:24, :] for c in range(3)]
    load = [in_forces[c] * load_scale for c in range(3)]
    put_sum(0, load[0] * precond[0] + load[1] * precond[1] + load[2] * precond[2])
    put_sum(1, image[0] * precond[0] + image[1] * precond[1] + image[2] * precond[2])
    unit_products(3, 6)
    finish_halo(4, fields.at[2], low_all.at[2], high_all.at[2], copies, plain)
    image_smooth = stiffness(2)
    change = []
    for c in range(3):
        remain = keep[c] - image_smooth[c]
        put_sum(2 + c, remain)
        change.append(fields[2, c, 1:5, 8:24, :] + dinv_buf[c] * remain)
    set_field(3, change)
    copies = start_halo(5, fields.at[3], change, plain)
    put_sum(5, dot3([keep[c] for c in range(3)], change))
    unit_products(6, 9)
    finish_halo(5, fields.at[3], low_all.at[3], high_all.at[3], copies, plain)
    image_change = stiffness(3)
    put_sum(6, dot3(image_change, [fields[3, c, 1:5, 8:24, :] for c in range(3)]))
    for j in range(9):
        put_sum(7 + j, dot3(image_change, [units[j, c] for c in range(3)]))
    rows_begin(1, make_row())
    rows_middle(1)
    rows_end(1)

    table = slab_rows(1)
    row = [table[q : q + 1, :] for q in range(FIRST_G)]
    solved = solve_again(stack3(row[2], row[3], row[4]))
    around = [pltpu.roll(solved, 1, 1), solved, pltpu.roll(solved, LANES - 1, 1)]
    at = [around[b][c : c + 1, :] for b in range(3) for c in range(3)]
    mixed = row[6]
    for i in range(9):
        inner = 2.0 * row[7 + i]
        for j in range(i + 1):
            q = FIRST_G + 9 * i + j
            inner = inner + (2.0 if j < i else 1.0) * table[q : q + 1, :] * at[j]
        mixed = mixed + at[i] * inner
    cross = row[5] + row[2] * at[3] + row[3] * at[4] + row[4] * at[5]

    def over_slabs(value):
        return jnp.sum(value, axis=1, keepdims=True)

    norm_now, curve = (over_slabs(row[0]), over_slabs(row[1]))
    cross, mixed = (over_slabs(cross), over_slabs(mixed))
    step0 = norm_now / curve
    norm_next = step0 * step0 * cross - norm_now
    curve_next = curve - 2.0 * step0 * cross + step0 * step0 * mixed
    ratio = norm_next / norm_now
    step1 = norm_next / (curve_next - ratio * norm_next / step0)
    near = nearby(solved)
    wide0 = jnp.broadcast_to(step0, (32, LANES))
    for target, extra in zip((fields, low_all, high_all), coarse_fields(near)):
        for c in range(3):
            target[3, c] = target[1, c] - wide0 * (target[3, c] + extra[c])
    image_next = stiffness(3)
    wide0 = jnp.broadcast_to(step0, (16, LANES))
    wide_ratio = jnp.broadcast_to(ratio, (16, LANES))
    wide1 = jnp.broadcast_to(step1, (16, LANES))
    for c in range(3):
        previous = fields[1, c, 1:5, 8:24, :]
        search = fields[3, c, 1:5, 8:24, :] + wide_ratio * previous
        disp_out[c] = wide0 * previous + wide1 * search
        residual = in_forces[c] * load_scale - wide0 * keep[c]
        res_out[c] = residual - wide1 * (image_next[c] + wide_ratio * keep[c])


def solution(mesh):
    sizes = tuple(mesh.shape[name] for name in ("gx", "gy", "gz"))
    n_gx, n_gy, n_gz = sizes
    n_group = n_gy * n_gz
    block = jax.ShapeDtypeStruct((3, 4, 16, LANES), F32)
    vmem = pl.BlockSpec(memory_space=pltpu.VMEM)

    def body(density, fixed_mask, load_mask, forces):
        def run(*refs):
            kernel(sizes, *refs)

        return pl.pallas_call(
            run,
            out_shape=(block, block),
            in_specs=[pl.BlockSpec(memory_space=pl.ANY)] * 4,
            out_specs=(vmem, vmem),
            scratch_shapes=[
                pltpu.VMEM((1, 6, 32, LANES), F32),
                pltpu.VMEM((N_FIELD, 3, 6, 32, LANES), F32),
                pltpu.VMEM((N_FIELD, 3, 6, 32, LANES), F32),
                pltpu.VMEM((N_FIELD, 3, 6, 32, LANES), F32),
                pltpu.VMEM((1, 6, 32, LANES), F32),
                pltpu.VMEM((1, 6, 32, LANES), F32),
                pltpu.VMEM((N_BASIS, 6, 32, LANES), F32),
                pltpu.VMEM((N_BASIS, 6, 32, LANES), F32),
                pltpu.VMEM((N_BASIS, 6, 32, LANES), F32),
                pltpu.VMEM((N_EX, 2, 8, LANES), F32),
                pltpu.VMEM((N_EX, 5, 8, LANES), F32),
                pltpu.VMEM((N_EX, 1, 8, LANES), F32),
                pltpu.VMEM((4, 8, LANES), F32),
                pltpu.VMEM((5, 24, LANES), F32),
                pltpu.VMEM((7, 4, 16, LANES), F32),
                pltpu.VMEM((3, 4, 16, LANES), F32),
                pltpu.VMEM((3, 4, 16, LANES), F32),
                pltpu.VMEM((N_ROWS, LANES), F32),
                pltpu.VMEM((9, 3, 4, 16, LANES), F32),
                pltpu.VMEM((steps_for(n_gx) + 1, 6, 8, LANES), F32),
                pltpu.VMEM((2, 2, 1, LANES), F32),
                pltpu.VMEM((2, n_group, 1, LANES), F32),
                pltpu.VMEM((2, n_gx, 1, LANES), F32),
                pltpu.VMEM((4, 16, LANES), jnp.int32),
                pltpu.VMEM((4, 16, LANES), jnp.int32),
                pltpu.VMEM((4, 16, LANES), jnp.int32),
                pltpu.VMEM((3, 4, 16, LANES), F32),
                pltpu.SemaphoreType.DMA((4,)),
                pltpu.SemaphoreType.DMA((N_EX, N_MSG)),
                pltpu.SemaphoreType.DMA((N_EX, N_MSG)),
                pltpu.SemaphoreType.DMA((2, 2)),
                pltpu.SemaphoreType.DMA((2, 2)),
                pltpu.SemaphoreType.REGULAR((8, 2)),
            ],
            compiler_params=pltpu.CompilerParams(collective_id=0, has_side_effects=True),
        )(density, fixed_mask, load_mask, forces)

    spec = P("gx", "gy", "gz")
    wide = P(None, "gx", "gy", "gz")
    return jax.shard_map(
        body,
        mesh=mesh,
        in_specs=(spec, spec, spec, wide),
        out_specs=(wide, wide),
        check_vma=False,
    )
```

```python
import jax
import jax.numpy as jnp
from jax import lax
from jax.experimental import pallas as pl
from jax.experimental.pallas import tpu as pltpu
from jax.sharding import PartitionSpec as P

LAME = 0.5
PENALTY = 4.0
OMEGA = 0.5
F32 = jnp.float32
MESH = pl.DeviceIdType.MESH
LANES = 128
N_MSG = 9
N_EX = 6
N_FIELD = 5
N_ROWS = 104
FIRST_G = 16
N_BASIS = 10


def steps_for(count):
    steps = 0
    while (1 << steps) < count:
        steps += 1
    return steps


def kernel(
    sizes,
    density,
    fixed_mask,
    load_mask,
    forces,
    disp_out,
    res_out,
    mod_buf,
    fields,
    low_all,
    high_all,
    mod_low,
    mod_high,
    basis,
    basis_low,
    basis_high,
    pack_send,
    pack_recv,
    edge_recv,
    basis_edge,
    stress,
    coef,
    dinv_buf,
    keep,
    rows_buf,
    units,
    pcr_buf,
    row_send,
    group_recv,
    slab_recv,
    in_density,
    in_fixed,
    in_load,
    in_forces,
    in_sem,
    halo_send_sem,
    halo_recv_sem,
    row_send_sem,
    row_recv_sem,
    flood_sem,
):
    n_gx, n_gy, n_gz = sizes
    n_group = n_gy * n_gz
    gx, gy, gz = (lax.axis_index("gx"), lax.axis_index("gy"), lax.axis_index("gz"))

    def wrap(value, count):
        value = jnp.where(value >= count, value - count, value)
        return jnp.where(value < 0, value + count, value)

    gx_up, gx_dn = (wrap(gx + 1, n_gx), wrap(gx - 1, n_gx))
    gz_up, gz_dn = (wrap(gz + 1, n_gz), wrap(gz - 1, n_gz))
    gy_other = 1 - gy
    gx_side = wrap(gx + 2 * gy - 1, n_gx)
    gz_side = wrap(gz + 2 * gy - 1, n_gz)

    def group_member(step):
        y_at = jnp.where(step >= n_gz, gy_other, gy)
        z_at = wrap(gz + jnp.where(step >= n_gz, step - n_gz, step), n_gz)
        return (gx, y_at, z_at)

    barrier = pltpu.get_barrier_semaphore()

    def greet(where_to):
        pl.semaphore_signal(barrier, inc=1, device_id=where_to, device_id_type=MESH)

    near = [
        (gx_up, gy, gz),
        (gx_dn, gy, gz),
        (gx, gy, gz_up),
        (gx, gy, gz_dn),
        (gx, gy_other, gz),
        (gx_side, gy_other, gz),
        (gx_dn, gy, gz_up),
        (gx_up, gy, gz_dn),
        (gx, gy_other, gz_side),
    ]
    n_fast = 12 if n_gx == 48 else n_gx
    n_slow = n_gx // n_fast
    slow = gx // n_fast
    fast = gx - slow * n_fast
    ring_fast = [slow * n_fast + wrap(fast + d, n_fast) for d in (1, -1)]
    ring_slow = [wrap(slow + d, n_slow) * n_fast + fast for d in (1, -1)]
    if n_slow > 1:
        near = near + [(v, gy, gz) for v in ring_slow + ring_fast]
    for where_to in near:
        greet(where_to)
    fetches = []
    for k, (src, dst) in enumerate(
        ((density, in_density), (fixed_mask, in_fixed), (load_mask, in_load), (forces, in_forces))
    ):
        fetch = pltpu.make_async_copy(src, dst, in_sem.at[k])
        fetch.start()
        fetches.append(fetch)

    ring_y = [(gx, gy, gz_up), (gx, gy, gz_dn)]
    ring_z = [(v, gy, gz) for v in ring_fast]
    ring_x = [(v, gy, gz) for v in ring_slow]
    n_y, n_z = (max(n_gz // 2 - 1, 0), max(n_fast // 2 - 1, 0))
    floods = []
    for k in range(max(n_y, n_z)):
        floods.append(([ring_y] if k < n_y else []) + ([ring_z] if k < n_z else []))
    if n_slow > 1:
        floods += [[ring_x]] * max(n_slow // 2, 1)

    def flood(first, last):
        for k in range(first, min(last, len(floods))):
            for r, ring in enumerate(floods[k]):
                for where_to in ring:
                    pl.semaphore_signal(
                        flood_sem.at[k, r], inc=1, device_id=where_to, device_id_type=MESH
                    )
            for r in range(len(floods[k])):
                pl.semaphore_wait(flood_sem.at[k, r], 2)

    has_xm = jnp.where(gx > 0, 1.0, 0.0).astype(F32)
    has_xp = jnp.where(gx < n_gx - 1, 1.0, 0.0).astype(F32)
    has_zm = jnp.where(gz > 0, 1.0, 0.0).astype(F32)
    has_zp = jnp.where(gz < n_gz - 1, 1.0, 0.0).astype(F32)
    is_y0 = jnp.where(gy == 0, 1.0, 0.0).astype(F32)
    is_y1 = 1.0 - is_y0

    shape = (4, 16, LANES)
    lane3 = lax.broadcasted_iota(jnp.int32, shape, 2)
    x3 = lax.broadcasted_iota(jnp.int32, shape, 0)
    y3 = lax.broadcasted_iota(jnp.int32, shape, 1)
    slot3 = 2 * x3 + jnp.where(y3 >= 8, 1, 0)
    first_lane, last_lane = (lane3 == 0, lane3 == LANES - 1)
    wide_lane = lax.broadcasted_iota(jnp.int32, (5, 24, LANES), 2) == LANES - 1
    table_shape = (N_ROWS, LANES)
    diag2 = lax.broadcasted_iota(jnp.int32, table_shape, 1) == lax.broadcasted_iota(
        jnp.int32, table_shape, 0
    )

    zeros_side = jnp.zeros((4, 8, LANES), F32)
    outside = pl.ds(pl.multiple_of(24 * gy, 8), 8)
    padded = [(mod_buf, 1), (basis, N_BASIS)] + [(fields.at[e], 3) for e in range(4)]
    for buf, count in padded:
        for c in range(count):
            buf[c, 1:5, outside, :] = zeros_side

    for fetch in fetches:
        fetch.wait()
    level = in_density[...].astype(F32) / 15.0
    mod = 0.05 + 0.95 * level * level * level
    mod_buf[0, 1:5, 8:24, :] = mod
    fixed4 = PENALTY * in_fixed[...].astype(F32)
    load_scale = 0.25 + in_load[...].astype(F32)
    load = [in_forces[c] * load_scale for c in range(3)]

    def pack_side(values, lane):
        total = None
        for c, value in enumerate(values):
            spread = jnp.broadcast_to(value[:, :, lane : lane + 1], shape)
            chosen = jnp.where(lane3 == slot3 + 8 * c, spread, 0.0)
            flat = chosen[0] + chosen[1] + chosen[2] + chosen[3]
            part = flat[0:8] + flat[8:16]
            total = part if total is None else total + part
        return total

    def remote(e, k, src, dst, where_to):
        copy = pltpu.make_async_remote_copy(
            src_ref=src,
            dst_ref=dst,
            send_sem=halo_send_sem.at[e, k],
            recv_sem=halo_recv_sem.at[e, k],
            device_id=where_to,
            device_id_type=MESH,
        )
        copy.start()
        return copy

    def start_halo(e, buf, values, groups):
        edge = edge_recv.at[e] if len(values) <= 3 else basis_edge
        copies = [
            remote(e, 0, buf.at[:, 4, 8:24, :], buf.at[:, 0, 8:24, :], (gx_up, gy, gz)),
            remote(e, 1, buf.at[:, 1, 8:24, :], buf.at[:, 5, 8:24, :], (gx_dn, gy, gz)),
        ]
        pack_send[e, 0] = pack_side(values, LANES - 1)
        pack_send[e, 1] = pack_side(values, 0)
        copies.append(
            remote(e, 2, pack_send.at[e, 0], pack_recv.at[e, 0], (gx, gy, gz_up))
        )
        copies.append(
            remote(e, 3, pack_send.at[e, 1], pack_recv.at[e, 1], (gx, gy, gz_dn))
        )
        if groups is not None:
            copies.append(
                remote(e, 4, pack_send.at[e, 0], pack_recv.at[e, 2], (gx_dn, gy, gz_up))
            )
            copies.append(
                remote(e, 5, pack_send.at[e, 1], pack_recv.at[e, 3], (gx_up, gy, gz_dn))
            )
            copies.append(
                remote(
                    e, 6, pack_send.at[e, 1 - gy], pack_recv.at[e, 4], (gx, gy_other, gz_side)
                )
            )
            copies.append(
                remote(
                    e,
                    7,
                    buf.at[
                        pl.ds(len(groups[0]) * gy, len(groups[0])),
                        1 + 3 * gy,
                        pl.ds(pl.multiple_of(16 - 8 * gy, 8), 8),
                        :,
                    ],
                    edge,
                    (gx_side, gy_other, gz),
                )
            )
        copies.append(
            remote(
                e,
                8,
                buf.at[:, 1:5, pl.ds(pl.multiple_of(16 - 8 * gy, 8), 8), :],
                buf.at[:, 1:5, pl.ds(pl.multiple_of(24 * gy, 8), 8), :],
                (gx, gy_other, gz),
            )
        )
        return copies

    def finish_halo(e, buf, low_to, high_to, copies, groups):
        for copy in copies:
            copy.wait()
        count = buf.shape[0]
        for c in range(count):
            buf[c, 0, 8:24, :] = buf[c, 0, 8:24, :] * has_xm
            buf[c, 5, 8:24, :] = buf[c, 5, 8:24, :] * has_xp

        def spread_to(target, c, x, rows, pack, j):
            target[c, x, rows, :] = jnp.broadcast_to(pack[:, j : j + 1], (8, LANES))

        low = pack_recv[e, 0] * has_zm
        high = pack_recv[e, 1] * has_zp
        tiles = [slice(8, 16), slice(16, 24)]
        for c in range(count):
            for x in range(4):
                for t in range(2):
                    spread_to(low_to, c, 1 + x, tiles[t], low, 8 * c + 2 * x + t)
                    spread_to(high_to, c, 1 + x, tiles[t], high, 8 * c + 2 * x + t)
        if groups is not None:
            of_x, of_y, of_z = groups
            low_x = pack_recv[e, 2] * (has_xp * has_zm)
            high_x = pack_recv[e, 3] * (has_xm * has_zp)
            side = pack_recv[e, 4]
            low_y = side * (is_y0 * has_zm)
            high_y = side * (is_y1 * has_zp)
            for t in range(2):
                for c in of_x:
                    spread_to(low_to, c, 5, tiles[t], low_x, 8 * c + t)
                for c in of_z:
                    spread_to(high_to, c, 0, tiles[t], high_x, 8 * c + 6 + t)
            for x in range(4):
                for c in of_y:
                    spread_to(low_to, c, 1 + x, slice(24, 32), low_y, 8 * c + 2 * x)
                for c in of_z:
                    spread_to(high_to, c, 1 + x, slice(0, 8), high_y, 8 * c + 2 * x + 1)
            edge = edge_recv.at[e] if count <= 3 else basis_edge
            for k, c in enumerate(of_y):
                buf[c, 0, 24:32, :] = edge[k] * (is_y0 * has_xm)
            for k, c in enumerate(of_x):
                buf[c, 5, 0:8, :] = edge[k] * (is_y1 * has_xp)

    def before(value, low):
        return jnp.where(first_lane, low, pltpu.roll(value, 1, 2))

    def after(value, high):
        return jnp.where(last_lane, high, pltpu.roll(value, LANES - 1, 2))

    def set_field(e, values):
        for c in range(3):
            fields[e, c, 1:5, 8:24, :] = values[c]

    def stiffness(e):
        buf, low_z, high_z = (fields.at[e], low_all.at[e], high_all.at[e])
        u_z = buf[2, 0:5, 0:24, :]
        up_z = jnp.where(wide_lane, high_z[2, 0:5, 0:24, :], pltpu.roll(u_z, LANES - 1, 2))
        spread = (
            (buf[0, 1:6, 0:24, :] - buf[0, 0:5, 0:24, :])
            + (buf[1, 0:5, 1:25, :] - buf[1, 0:5, 0:24, :])
            + (up_z - u_z)
        )
        stress[...] = mod_buf[0, 0:5, 0:24, :] * spread
        here = stress[1:5, 8:24, :]
        spread_low = (
            (low_z[0, 2:6, 8:24, :] - low_z[0, 1:5, 8:24, :])
            + (low_z[1, 1:5, 9:25, :] - low_z[1, 1:5, 8:24, :])
            + (buf[2, 1:5, 8:24, :] - low_z[2, 1:5, 8:24, :])
        )
        below = [
            stress[0:4, 8:24, :],
            stress[1:5, 7:23, :],
            before(here, mod_low[0, 1:5, 8:24, :] * spread_low),
        ]
        images = []
        for c in range(3):
            centre = buf[c, 1:5, 8:24, :]
            image = coef[6] * centre
            image = image - coef[0] * buf[c, 0:4, 8:24, :]
            image = image - coef[1] * buf[c, 2:6, 8:24, :]
            image = image - coef[2] * buf[c, 1:5, 7:23, :]
            image = image - coef[3] * buf[c, 1:5, 9:25, :]
            image = image - coef[4] * before(centre, low_z[c, 1:5, 8:24, :])
            image = image - coef[5] * after(centre, high_z[c, 1:5, 8:24, :])
            images.append(image + LAME * (below[c] - here))
        return images

    def put_sum(q, value):
        if value.ndim == 3:
            value = value[0] + value[1] + value[2] + value[3]
        value = value[0:8] + value[8:16]
        rows_buf[pl.ds(q, 1), :] = jnp.sum(value, axis=0, keepdims=True)

    def make_row():
        sums = jnp.sum(rows_buf[...], axis=1, keepdims=True)
        return jnp.sum(jnp.where(diag2, sums, 0.0), axis=0, keepdims=True)

    me_group = gy * n_gz + gz

    def far_first(step):
        return wrap(step + n_gx // 2, n_gx - 1) + 1

    def rows_begin(i, row):
        row_send[i, 0] = row
        group_recv[i, me_group] = row

        def group_copy(step):
            return pltpu.make_async_remote_copy(
                src_ref=row_send.at[i, 0],
                dst_ref=group_recv.at[i, me_group],
                send_sem=row_send_sem.at[i, 0],
                recv_sem=row_recv_sem.at[i, 0],
                device_id=group_member(step),
                device_id_type=MESH,
            )

        def start_group(step, carry):
            group_copy(step).start()
            return carry

        lax.fori_loop(1, n_group, start_group, 0, unroll=True)

    def rows_middle(i):
        most = group_recv.at[i, pl.ds(0, n_group - 1)]
        pltpu.make_async_copy(most, most, row_recv_sem.at[i, 0]).wait()
        total = group_recv[i, 0]
        for k in range(1, n_group):
            total = total + group_recv[i, k]
        row_send[i, 1] = total
        slab_recv[i, gx] = total

        def start_slab(step, carry):
            pltpu.make_async_remote_copy(
                src_ref=row_send.at[i, 1],
                dst_ref=slab_recv.at[i, gx],
                send_sem=row_send_sem.at[i, 1],
                recv_sem=row_recv_sem.at[i, 1],
                device_id=(wrap(gx + far_first(step), n_gx), gy, gz),
                device_id_type=MESH,
            ).start()
            return carry

        lax.fori_loop(0, n_gx - 1, start_slab, 0, unroll=True)

    def rows_end(i):
        most = group_recv.at[i, pl.ds(0, n_group - 1)]
        rest = slab_recv.at[i, pl.ds(0, n_gx - 1)]
        pltpu.make_async_copy(rest, rest, row_recv_sem.at[i, 1]).wait()
        pltpu.make_async_copy(most, most, row_send_sem.at[i, 0]).wait()
        pltpu.make_async_copy(rest, rest, row_send_sem.at[i, 1]).wait()

    def slab_rows(i):
        table = jnp.concatenate(
            [slab_recv[i, k] for k in range(n_gx)]
            + [jnp.zeros((LANES - n_gx, LANES), F32)],
            axis=0,
        )
        return jnp.transpose(table)

    lane_row = lax.broadcasted_iota(jnp.int32, (1, LANES), 1)
    sub8 = lax.broadcasted_iota(jnp.int32, (8, LANES), 0)
    n_steps = steps_for(n_gx)

    def stack3(a, b, c):
        return jnp.where(sub8 == 0, a, jnp.where(sub8 == 1, b, jnp.where(sub8 == 2, c, 0.0)))

    def times(matrix, column):
        return (
            matrix[0] * column[0:1, :] + matrix[1] * column[1:2, :] + matrix[2] * column[2:3, :]
        )

    def inverse(cols):
        a, d, g = (cols[0][0:1, :], cols[0][1:2, :], cols[0][2:3, :])
        b, e, h = (cols[1][0:1, :], cols[1][1:2, :], cols[1][2:3, :])
        c, f, i = (cols[2][0:1, :], cols[2][1:2, :], cols[2][2:3, :])
        m00, m01, m02 = (e * i - f * h, c * h - b * i, b * f - c * e)
        m10, m11, m12 = (f * g - d * i, a * i - c * g, c * d - a * f)
        m20, m21, m22 = (d * h - e * g, b * g - a * h, a * e - b * d)
        scale = 1.0 / (a * m00 + b * m10 + c * m20)
        return [
            stack3(m00 * scale, m10 * scale, m20 * scale),
            stack3(m01 * scale, m11 * scale, m21 * scale),
            stack3(m02 * scale, m12 * scale, m22 * scale),
        ]

    def factorise(lower, main, upper, rhs):
        def body(step, carry):
            stride, low, mid, high, vec = carry
            back = LANES - stride
            inv = inverse(mid)
            inv_dn = [pltpu.roll(v, stride, 1) for v in inv]
            inv_up = [pltpu.roll(v, back, 1) for v in inv]
            alpha = [-times(low, v) for v in inv_dn]
            gamma = [-times(high, v) for v in inv_up]
            for k in range(3):
                pcr_buf[step, k] = alpha[k]
                pcr_buf[step, 3 + k] = gamma[k]
            low_dn = [pltpu.roll(v, stride, 1) for v in low]
            high_dn = [pltpu.roll(v, stride, 1) for v in high]
            low_up = [pltpu.roll(v, back, 1) for v in low]
            high_up = [pltpu.roll(v, back, 1) for v in high]
            vec_dn = pltpu.roll(vec, stride, 1)
            vec_up = pltpu.roll(vec, back, 1)
            new_mid = [
                mid[k] + times(alpha, high_dn[k]) + times(gamma, low_up[k]) for k in range(3)
            ]
            new_low = [times(alpha, v) for v in low_dn]
            new_high = [times(gamma, v) for v in high_up]
            new_vec = vec + times(alpha, vec_dn) + times(gamma, vec_up)
            return (stride * 2, new_low, new_mid, new_high, new_vec)

        _, _, mid, _, vec = lax.fori_loop(
            0, n_steps, body, (jnp.int32(1), lower, main, upper, rhs)
        )
        inv = inverse(mid)
        for k in range(3):
            pcr_buf[n_steps, k] = inv[k]
        return times(inv, vec)

    def solve_again(vec):
        stride = 1
        for step in range(n_steps):
            alpha = [pcr_buf[step, k] for k in range(3)]
            gamma = [pcr_buf[step, 3 + k] for k in range(3)]
            vec_dn = pltpu.roll(vec, stride, 1)
            vec_up = pltpu.roll(vec, LANES - stride, 1)
            vec = vec + times(alpha, vec_dn) + times(gamma, vec_up)
            stride *= 2
        return times([pcr_buf[n_steps, k] for k in range(3)], vec)

    def nearby(solved):
        turned = pltpu.roll(solved, wrap(1 - gx, LANES), 1)
        return [
            [jnp.broadcast_to(turned[c : c + 1, b : b + 1], (32, LANES)) for c in range(3)]
            for b in range(3)
        ]

    pl.semaphore_wait(barrier, len(near))

    plain = ((0,), (1,), (2,))
    copies = start_halo(0, mod_buf, [mod], None)
    flood(0, 4)
    finish_halo(0, mod_buf, mod_low, mod_high, copies, None)
    mod_zm = before(mod, mod_low[0, 1:5, 8:24, :])
    mod_zp = after(mod, mod_high[0, 1:5, 8:24, :])
    mod_xm, mod_xp = (mod_buf[0, 0:4, 8:24, :], mod_buf[0, 2:6, 8:24, :])
    mod_ym, mod_yp = (mod_buf[0, 1:5, 7:23, :], mod_buf[0, 1:5, 9:25, :])
    couplings = [0.5 * (mod + v) for v in (mod_xm, mod_xp, mod_ym, mod_yp, mod_zm, mod_zp)]
    total = fixed4
    for k in range(6):
        coef[k] = couplings[k]
        total = total + couplings[k]
    coef[6] = total
    for c in range(3):
        dinv_buf[c] = OMEGA / (total + couplings[2 * c])

    first = [load[c] * dinv_buf[c] for c in range(3)]
    set_field(0, first)
    copies = start_halo(1, fields.at[0], first, plain)
    flood(4, len(floods))

    low_y_edge = jnp.where(y3 == 0, is_y0, 0.0)
    high_y_edge = jnp.where(y3 == 15, is_y1, 0.0)
    low_z_edge = jnp.where(first_lane, 1.0 - has_zm, 0.0)
    high_z_edge = jnp.where(last_lane, 1.0 - has_zp, 0.0)
    first_x = jnp.where(x3 == 0, 1.0, 0.0)
    last_x = jnp.where(x3 == 3, 1.0, 0.0)
    bound = (
        fixed4
        + couplings[2] * low_y_edge
        + couplings[3] * high_y_edge
        + couplings[4] * low_z_edge
        + couplings[5] * high_z_edge
        + couplings[0] * first_x
        + couplings[1] * last_x
    )
    half = LAME * mod
    half_xm = LAME * mod_xm
    rows_buf[...] = jnp.zeros(table_shape, F32)
    put_sum(0, bound + half_xm * first_x + half * last_x)
    put_sum(1, bound + half * high_y_edge)
    put_sum(2, bound + half * high_z_edge)
    put_sum(3, half[3] * high_y_edge[3])
    put_sum(4, half[3] * high_z_edge[3])
    put_sum(5, half * high_y_edge * high_z_edge)
    put_sum(6, couplings[1][3])
    put_sum(7, couplings[1][3] + half[3])

    dinv = [dinv_buf[c] for c in range(3)]
    inner_xm = half_xm * (1.0 - first_x)
    pieces = [
        dinv[0] * (bound + half_xm * first_x + half * last_x),
        dinv[0] * (half - inner_xm),
        dinv[0] * (first_x * (couplings[0] + half_xm) + last_x * (couplings[1] + half)),
        dinv[0] * first_x * half_xm,
        dinv[1] * (bound + half * high_y_edge),
        dinv[1] * (half - LAME * mod_ym),
        dinv[1] * (first_x * couplings[0] + last_x * couplings[1]),
        dinv[2] * (bound + half * high_z_edge),
        dinv[2] * (half - LAME * mod_zm),
        dinv[2] * (first_x * couplings[0] + last_x * couplings[1]),
    ]
    for c in range(N_BASIS):
        basis[c, 1:5, 8:24, :] = pieces[c]
    basis_groups = ((0, 1, 2, 3), (4, 5, 6), (7, 8, 9))

    whole = (6, 32, LANES)
    x6 = lax.broadcasted_iota(jnp.int32, whole, 0)
    y6 = lax.broadcasted_iota(jnp.int32, whole, 1)
    lane6 = lax.broadcasted_iota(jnp.int32, whole, 2)

    def coarse_fields(near):
        under, here, over = near
        inside = jnp.where(y6 < 8, is_y1, jnp.where(y6 >= 24, is_y0, 1.0))
        top_y = jnp.where(y6 == 23, is_y1, 0.0)
        top_z = jnp.where(lane6 == LANES - 1, 1.0 - has_zp, 0.0)
        own = [jnp.where(x6 == 0, under[c], jnp.where(x6 == 5, over[c], here[c])) for c in range(3)]
        other = [
            jnp.where(
                x6 == 1,
                under[c],
                jnp.where(
                    x6 == 4, over[c], jnp.where(jnp.logical_or(x6 == 0, x6 == 5), here[c], 0.0)
                ),
            )
            for c in range(3)
        ]
        drop = jnp.where(x6 == 4, here[0] - over[0], jnp.where(x6 == 0, under[0] - here[0], 0.0))
        own_y, other_y = (top_y * own[1], top_y * other[1])
        own_z, other_z = (top_z * own[2], top_z * other[2])

        def evaluate(b, scale, with_z):
            t_own = own_y + own_z if with_z else own_y
            t_other = other_y + other_z if with_z else other_y
            drop_y = drop + own_z if with_z else drop
            held = inside if scale is None else inside * scale
            return [
                (held - b[0]) * own[0] - b[1] * t_own + b[2] * other[0] + b[3] * t_other,
                (held - b[4]) * own[1] - b[5] * drop_y + b[6] * other[1],
                (held - b[7]) * own[2] - b[8] * (drop + own_y) + b[9] * other[2],
            ]

        return (
            evaluate(basis, None, True),
            evaluate(basis_low, has_zm, False),
            evaluate(basis_high, has_zp, False),
        )

    def dot3(left, right):
        return left[0] * right[0] + left[1] * right[1] + left[2] * right[2]

    def unit_products(first_unit, last_unit):
        def body(i, carry):
            near = [
                [
                    jnp.broadcast_to(jnp.where(i == 3 * b + c, 1.0, 0.0).astype(F32), (32, LANES))
                    for c in range(3)
                ]
                for b in range(3)
            ]
            for target, value in zip((fields, low_all, high_all), coarse_fields(near)):
                for c in range(3):
                    target[4, c] = value[c]
            for c in range(3):
                units[i, c] = fields[4, c, 1:5, 8:24, :]
            image = stiffness(4)
            for j in range(9):
                put_sum(FIRST_G + 9 * i + j, dot3(image, [units[j, c] for c in range(3)]))
            return carry

        lax.fori_loop(first_unit, last_unit, body, 0)

    units[...] = jnp.zeros((9, 3, 4, 16, LANES), F32)
    finish_halo(1, fields.at[0], low_all.at[0], high_all.at[0], copies, plain)
    image_first = stiffness(0)
    rest = [load[c] - image_first[c] for c in range(3)]
    for c in range(3):
        put_sum(8 + c, rest[c])
    rows_begin(0, make_row())
    partial = [first[c] + dinv_buf[c] * rest[c] for c in range(3)]
    set_field(1, partial)
    copies = start_halo(2, fields.at[1], partial, plain)
    more = start_halo(3, basis, [basis[c, 1:5, 8:24, :] for c in range(N_BASIS)], basis_groups)
    rows_middle(0)
    finish_halo(2, fields.at[1], low_all.at[1], high_all.at[1], copies, plain)
    finish_halo(3, basis, basis_low, basis_high, more, basis_groups)
    unit_products(0, 3)
    rows_end(0)

    table = slab_rows(0)
    real = lane_row < n_gx
    row = [jnp.where(real, table[q : q + 1, :], 0.0) for q in range(11)]
    one = jnp.where(real, 0.0, 1.0)
    none = jnp.zeros((1, LANES), F32)
    main = [
        stack3(row[0] + one, row[3], row[4]),
        stack3(row[3], row[1] + one, row[5]),
        stack3(row[4], row[5], row[2] + one),
    ]
    joined = lane_row < n_gx - 1
    side = [jnp.where(joined, row[q], 0.0) for q in (7, 3, 4, 6)]
    upper = [
        stack3(-side[0], -side[1], -side[2]),
        stack3(none, -side[3], none),
        stack3(none, none, -side[3]),
    ]
    moved = [pltpu.roll(jnp.broadcast_to(v, (8, LANES)), 1, 1)[0:1, :] for v in side]
    lower = [
        stack3(-moved[0], none, none),
        stack3(-moved[1], -moved[3], none),
        stack3(-moved[2], none, -moved[3]),
    ]
    near = nearby(factorise(lower, main, upper, stack3(row[8], row[9], row[10])))
    for target, extra in zip((fields, low_all, high_all), coarse_fields(near)):
        for c in range(3):
            target[1, c] = target[1, c] + extra[c]
    image = stiffness(1)
    smooth = []
    for c in range(3):
        keep[c] = image[c]
        smooth.append(dinv_buf[c] * image[c])
    set_field(2, smooth)
    copies = start_halo(4, fields.at[2], smooth, plain)
    precond = [fields[1, c, 1:5, 8:24, :] for c in range(3)]
    load = [in_forces[c] * load_scale for c in range(3)]
    put_sum(0, load[0] * precond[0] + load[1] * precond[1] + load[2] * precond[2])
    put_sum(1, image[0] * precond[0] + image[1] * precond[1] + image[2] * precond[2])
    unit_products(3, 6)
    finish_halo(4, fields.at[2], low_all.at[2], high_all.at[2], copies, plain)
    image_smooth = stiffness(2)
    change = []
    for c in range(3):
        remain = keep[c] - image_smooth[c]
        put_sum(2 + c, remain)
        change.append(fields[2, c, 1:5, 8:24, :] + dinv_buf[c] * remain)
    set_field(3, change)
    copies = start_halo(5, fields.at[3], change, plain)
    put_sum(5, dot3([keep[c] for c in range(3)], change))
    unit_products(6, 9)
    finish_halo(5, fields.at[3], low_all.at[3], high_all.at[3], copies, plain)
    image_change = stiffness(3)
    put_sum(6, dot3(image_change, [fields[3, c, 1:5, 8:24, :] for c in range(3)]))
    for j in range(9):
        put_sum(7 + j, dot3(image_change, [units[j, c] for c in range(3)]))
    rows_begin(1, make_row())
    rows_middle(1)
    rows_end(1)

    table = slab_rows(1)
    row = [table[q : q + 1, :] for q in range(FIRST_G)]
    solved = solve_again(stack3(row[2], row[3], row[4]))
    around = [pltpu.roll(solved, 1, 1), solved, pltpu.roll(solved, LANES - 1, 1)]
    at = [around[b][c : c + 1, :] for b in range(3) for c in range(3)]
    mixed = row[6]
    for i in range(9):
        inner = 2.0 * row[7 + i]
        for j in range(i + 1):
            q = FIRST_G + 9 * i + j
            inner = inner + (2.0 if j < i else 1.0) * table[q : q + 1, :] * at[j]
        mixed = mixed + at[i] * inner
    cross = row[5] + row[2] * at[3] + row[3] * at[4] + row[4] * at[5]

    def over_slabs(value):
        return jnp.sum(value, axis=1, keepdims=True)

    norm_now, curve = (over_slabs(row[0]), over_slabs(row[1]))
    cross, mixed = (over_slabs(cross), over_slabs(mixed))
    step0 = norm_now / curve
    norm_next = step0 * step0 * cross - norm_now
    curve_next = curve - 2.0 * step0 * cross + step0 * step0 * mixed
    ratio = norm_next / norm_now
    step1 = norm_next / (curve_next - ratio * norm_next / step0)
    near = nearby(solved)
    wide0 = jnp.broadcast_to(step0, (32, LANES))
    for target, extra in zip((fields, low_all, high_all), coarse_fields(near)):
        for c in range(3):
            target[3, c] = target[1, c] - wide0 * (target[3, c] + extra[c])
    image_next = stiffness(3)
    wide0 = jnp.broadcast_to(step0, (16, LANES))
    wide_ratio = jnp.broadcast_to(ratio, (16, LANES))
    wide1 = jnp.broadcast_to(step1, (16, LANES))
    for c in range(3):
        previous = fields[1, c, 1:5, 8:24, :]
        search = fields[3, c, 1:5, 8:24, :] + wide_ratio * previous
        disp_out[c] = wide0 * previous + wide1 * search
        residual = in_forces[c] * load_scale - wide0 * keep[c]
        res_out[c] = residual - wide1 * (image_next[c] + wide_ratio * keep[c])


def solution(mesh):
    sizes = tuple(mesh.shape[name] for name in ("gx", "gy", "gz"))
    n_gx, n_gy, n_gz = sizes
    n_group = n_gy * n_gz
    place = pltpu.VMEM((3, 4, 16, LANES), F32)
    vmem = pl.BlockSpec(memory_space=pltpu.VMEM)

    def body(density, fixed_mask, load_mask, forces):
        def run(*refs):
            kernel(sizes, *refs)

        return pl.pallas_call(
            run,
            out_shape=(place, place),
            in_specs=[pl.BlockSpec(memory_space=pl.ANY)] * 4,
            out_specs=(vmem, vmem),
            scratch_shapes=[
                pltpu.VMEM((1, 6, 32, LANES), F32),
                pltpu.VMEM((N_FIELD, 3, 6, 32, LANES), F32),
                pltpu.VMEM((N_FIELD, 3, 6, 32, LANES), F32),
                pltpu.VMEM((N_FIELD, 3, 6, 32, LANES), F32),
                pltpu.VMEM((1, 6, 32, LANES), F32),
                pltpu.VMEM((1, 6, 32, LANES), F32),
                pltpu.VMEM((N_BASIS, 6, 32, LANES), F32),
                pltpu.VMEM((N_BASIS, 6, 32, LANES), F32),
                pltpu.VMEM((N_BASIS, 6, 32, LANES), F32),
                pltpu.VMEM((N_EX, 2, 8, LANES), F32),
                pltpu.VMEM((N_EX, 5, 8, LANES), F32),
                pltpu.VMEM((N_EX, 1, 8, LANES), F32),
                pltpu.VMEM((4, 8, LANES), F32),
                pltpu.VMEM((5, 24, LANES), F32),
                pltpu.VMEM((7, 4, 16, LANES), F32),
                pltpu.VMEM((3, 4, 16, LANES), F32),
                pltpu.VMEM((3, 4, 16, LANES), F32),
                pltpu.VMEM((N_ROWS, LANES), F32),
                pltpu.VMEM((9, 3, 4, 16, LANES), F32),
                pltpu.VMEM((steps_for(n_gx) + 1, 6, 8, LANES), F32),
                pltpu.VMEM((2, 2, 1, LANES), F32),
                pltpu.VMEM((2, n_group, 1, LANES), F32),
                pltpu.VMEM((2, n_gx, 1, LANES), F32),
                pltpu.VMEM((4, 16, LANES), jnp.int32),
                pltpu.VMEM((4, 16, LANES), jnp.int32),
                pltpu.VMEM((4, 16, LANES), jnp.int32),
                pltpu.VMEM((3, 4, 16, LANES), F32),
                pltpu.SemaphoreType.DMA((4,)),
                pltpu.SemaphoreType.DMA((N_EX, N_MSG)),
                pltpu.SemaphoreType.DMA((N_EX, N_MSG)),
                pltpu.SemaphoreType.DMA((2, 2)),
                pltpu.SemaphoreType.DMA((2, 2)),
                pltpu.SemaphoreType.REGULAR((8, 2)),
            ],
            compiler_params=pltpu.CompilerParams(collective_id=0, has_side_effects=True),
        )(density, fixed_mask, load_mask, forces)

    spec = P("gx", "gy", "gz")
    wide = P(None, "gx", "gy", "gz")
    return jax.shard_map(
        body,
        mesh=mesh,
        in_specs=(spec, spec, spec, wide),
        out_specs=(wide, wide),
        check_vma=False,
    )
```
